32 devices in a mesh: dp: 2 (over x), ty: 4 (over z), tx: 4 (over y, core).
Axes of the slice: x: 2, y: 2, z: 4, core: 2. Of those that a mesh axis runs over, the one named last changes fastest.
Arguments:
- x_in: bfloat16 [8, 512, 5120], P(('dp', 'ty'), None, 'tx'), parts along dimension 0
- w_q: bfloat16 [5120, 5120], P('tx', 'ty')
- w_k: bfloat16 [5120, 5120], P('tx', 'ty')
- w_v: bfloat16 [5120, 5120], P('tx', 'ty')
- w_o: bfloat16 [5120, 5120], P('ty', 'tx')
- w_gate: bfloat16 [5120, 13824], P('tx', 'ty')
- w_up: bfloat16 [5120, 13824], P('tx', 'ty')
- w_down: bfloat16 [13824, 5120], P('ty', 'tx')
Outputs:
- output: bfloat16 [8, 512, 5120], P(('dp', 'ty'), None, 'tx'), parts along dimension 0
There are 2 independent parts. The reference program is written for one: setup_inputs(seed, part) draws one part's arguments, and reference() takes and returns one part's arrays. A program takes and returns all parts, laid end to end along the dimension named above; an argument that names none is the same for every part.
All inputs are finite; a program needn't handle non-finite values.
Results may differ from the reference program's by a relative error of at most 0.0183301.
Values are sent between devices in bfloat16 or wider.
A program may use at most 1 GiB of HBM per device.

```python
import jax
import jax.numpy as jnp
from jax import lax

NSEQ = 4
SEQ = 512
D = 5120
FF = 13824
HEADS = 40

HEAD_DIM = D // HEADS
EPS = 1e-5
THETA = 10000.0


def setup_inputs(seed: int = 0, part: int = 0) -> dict:
    root_key = jax.random.key(seed)
    act_root, weight_root = jax.random.split(root_key)
    part_key = jax.random.fold_in(act_root, part)
    key_tok, key_scale, key_shift, key_slope, key_walk = jax.random.split(part_key, 5)
    tok_noise = jax.random.normal(key_tok, (NSEQ, SEQ, D), jnp.float32)
    tok_scale = jax.random.uniform(key_scale, (NSEQ, SEQ, 1), jnp.float32, 0.5, 2.0)
    tok_shift = 0.5 * jax.random.normal(key_shift, (NSEQ, SEQ, 1), jnp.float32)
    col_slope = jax.random.uniform(key_slope, (), jnp.float32, 1.0, 2.0)
    col_pos = jnp.arange(D, dtype=jnp.float32) / D - 0.5
    col_walk = jnp.cumsum(jax.random.normal(key_walk, (D,), jnp.float32)) * (1.5 * D ** -0.5)
    col_offset = 2.0 * col_slope * col_pos + col_walk
    x_in = (tok_scale * tok_noise + tok_shift + col_offset).astype(jnp.bfloat16)
    weight_keys = jax.random.split(weight_root, 7)

    def draw_weight(key_w, fan_in, fan_out, gain_mul):
        return (gain_mul * fan_in ** -0.5 * jax.random.normal(key_w, (fan_in, fan_out), jnp.float32)).astype(jnp.bfloat16)

    return {
        "x_in": x_in,
        "w_q": draw_weight(weight_keys[0], D, D, 1.5),
        "w_k": draw_weight(weight_keys[1], D, D, 1.5),
        "w_v": draw_weight(weight_keys[2], D, D, 1.0),
        "w_o": draw_weight(weight_keys[3], D, D, 2.5),
        "w_gate": draw_weight(weight_keys[4], D, FF, 1.0),
        "w_up": draw_weight(weight_keys[5], D, FF, 1.0),
        "w_down": draw_weight(weight_keys[6], FF, D, 2.0),
    }


def layer_norm(values_bf):
    values = values_bf.astype(jnp.float32)
    mean_val = jnp.mean(values, axis=-1, keepdims=True)
    var_val = jnp.mean(values * values, axis=-1, keepdims=True) - mean_val * mean_val
    return ((values - mean_val) * lax.rsqrt(var_val + EPS)).astype(jnp.bfloat16)


def rotary(heads_bf):
    seq_len = heads_bf.shape[1]
    half_dim = HEAD_DIM // 2
    inv_freq = THETA ** (-2.0 * jnp.arange(half_dim, dtype=jnp.float32) / HEAD_DIM)
    angles = jnp.arange(seq_len, dtype=jnp.float32)[:, None] * inv_freq[None, :]
    cos_t = jnp.cos(angles)[:, None, :]
    sin_t = jnp.sin(angles)[:, None, :]
    values = heads_bf.astype(jnp.float32)
    lower_half = values[..., :half_dim]
    upper_half = values[..., half_dim:]
    return jnp.concatenate([lower_half * cos_t - upper_half * sin_t, upper_half * cos_t + lower_half * sin_t], axis=-1).astype(jnp.bfloat16)


def causal_attention(q_heads, k_heads, v_heads):
    seq_len = q_heads.shape[1]
    q_block = min(seq_len, 128)
    key_pos = jnp.arange(seq_len)
    k_vals = k_heads.astype(jnp.float32)
    v_vals = v_heads.astype(jnp.float32)

    def one_block(block_idx, out_acc):
        q_start = block_idx * q_block
        q_blk = lax.dynamic_slice_in_dim(q_heads, q_start, q_block, axis=1).astype(jnp.float32)
        scores = jnp.einsum("nqhd,nkhd->nhqk", q_blk, k_vals) * HEAD_DIM ** -0.5
        q_pos = q_start + jnp.arange(q_block)
        allowed = q_pos[:, None] >= key_pos[None, :]
        scores = jnp.where(allowed, scores, -1e30)
        prob_blk = jax.nn.softmax(scores, axis=-1).astype(jnp.bfloat16).astype(jnp.float32)
        blk_out = jnp.einsum("nhqk,nkhd->nqhd", prob_blk, v_vals).astype(jnp.bfloat16)
        return lax.dynamic_update_slice_in_dim(out_acc, blk_out, q_start, axis=1)

    return lax.fori_loop(0, seq_len // q_block, one_block, jnp.zeros_like(q_heads))


def project(rows_bf, weight):
    return jnp.dot(rows_bf, weight, preferred_element_type=jnp.float32).astype(jnp.bfloat16)


def reference(x_in, w_q, w_k, w_v, w_o, w_gate, w_up, w_down):
    n_seqs, seq_len, d_model = x_in.shape
    head_shape = (n_seqs, seq_len, HEADS, HEAD_DIM)
    x_rows = x_in.reshape(n_seqs * seq_len, d_model)
    normed = layer_norm(x_rows)
    q_heads = rotary(project(normed, w_q).reshape(head_shape))
    k_heads = rotary(project(normed, w_k).reshape(head_shape))
    v_heads = project(normed, w_v).reshape(head_shape)
    attn_heads = causal_attention(q_heads, k_heads, v_heads)
    attn_out = project(attn_heads.reshape(n_seqs * seq_len, d_model), w_o)
    resid_h = (x_rows.astype(jnp.float32) + attn_out.astype(jnp.float32)).astype(jnp.bfloat16)
    normed_mlp = layer_norm(resid_h)
    gate_val = project(normed_mlp, w_gate)
    up_val = project(normed_mlp, w_up)
    act_val = (jax.nn.silu(gate_val.astype(jnp.float32)) * up_val.astype(jnp.float32)).astype(jnp.bfloat16)
    mlp_out = project(act_val, w_down)
    y_out = (resid_h.astype(jnp.float32) + mlp_out.astype(jnp.float32)).astype(jnp.bfloat16)
    return y_out.reshape(n_seqs, seq_len, d_model)
```

```python
import jax
import jax.numpy as jnp
from jax import lax
from jax.sharding import PartitionSpec as P

HEAD_DIM = 128
EPS = 1e-5
THETA = 10000.0
CHUNKS = 2
BF = jnp.bfloat16
F32 = jnp.float32


def rot_tables(start, rows):
    half_dim = HEAD_DIM // 2
    inv_freq = THETA ** (-2.0 * jnp.arange(half_dim, dtype=F32) / HEAD_DIM)
    angles = (start + jnp.arange(rows, dtype=F32))[:, None] * inv_freq[None, :]
    cos_t, sin_t = jnp.cos(angles), jnp.sin(angles)
    return jnp.concatenate([cos_t, cos_t], -1), jnp.concatenate([-sin_t, sin_t], -1)


def rotary(vals, tables):
    cos_t, sin_t = tables
    swapped = jnp.concatenate([vals[..., HEAD_DIM // 2:], vals[..., :HEAD_DIM // 2]], axis=-1)
    return (vals * cos_t[:, None, :] + swapped * sin_t[:, None, :]).astype(BF)


def attend(q, k, v, start):
    rows, keys = q.shape[1], k.shape[1]
    scores = jnp.einsum("nqhd,nkhd->nhqk", q, k, preferred_element_type=F32) * HEAD_DIM ** -0.5
    allowed = (start + jnp.arange(rows))[:, None] >= jnp.arange(keys)[None, :]
    scores = jnp.where(allowed, scores, -1e30)
    prob = jax.nn.softmax(scores, axis=-1).astype(BF)
    return jnp.einsum("nhqk,nkhd->nqhd", prob, v, preferred_element_type=F32).astype(BF)


def dot32(rows, weight):
    return jnp.einsum("...c,ch->...h", rows, weight, preferred_element_type=F32)


def moments(vals):
    return jnp.stack([jnp.sum(vals, axis=-1), jnp.sum(vals * vals, axis=-1)], axis=-1)


def normed(vals, sums, full_width):
    mean_val = sums[..., 0:1] / full_width
    var_val = sums[..., 1:2] / full_width - mean_val * mean_val
    return ((vals - mean_val) * lax.rsqrt(var_val + EPS)).astype(BF)


def xor_order(parts, me):
    parts = jnp.where(me % 2 == 1, jnp.stack([parts[1], parts[0], parts[3], parts[2]]), parts)
    return jnp.where(me >= 2, jnp.stack([parts[2], parts[3], parts[0], parts[1]]), parts)


def solution(mesh):
    tx_count = mesh.shape["tx"]
    act_spec = P(("dp", "ty"), None, "tx")
    col_spec = P("tx", "ty")
    row_spec = P("ty", "tx")
    core_pairs = [(i, i ^ 1) for i in range(4)]
    y_pairs = [(i, i ^ 2) for i in range(4)]

    def to_core(val):
        return lax.ppermute(val, "tx", core_pairs)

    def to_y(val):
        return lax.ppermute(val, "tx", y_pairs)

    def layer_fn(x_blk, w_q, w_k, w_v, w_o, w_gate, w_up, w_down):
        me = lax.axis_index("tx")
        core, ypos = me % 2, me // 2
        seq_len, width = x_blk.shape[1:]
        full_width = width * tx_count
        n_seqs = lax.axis_size("ty")
        own_seqs = n_seqs // 2
        rows = seq_len // CHUNKS
        quarter = rows // 4
        heads = w_q.shape[1] // HEAD_DIM
        half_cols = w_q.shape[1] // 2
        x32 = x_blk[0].astype(F32)
        n1 = normed(x32, lax.psum(moments(x32), "tx"), full_width)

        k_parts, v_parts, attn_sent = [], [], []
        for j in range(CHUNKS):
            gathered = lax.all_gather(n1[j * rows:(j + 1) * rows], "ty", axis=0)
            mine = lax.dynamic_slice_in_dim(gathered, own_seqs * core, own_seqs, 0)
            other = lax.dynamic_slice_in_dim(gathered, own_seqs * (1 - core), own_seqs, 0)
            done = []
            for w in (w_k, w_q, w_v):
                got = to_core(dot32(other, w).astype(BF))
                chip_sum = (dot32(mine, w) + got.astype(F32)).astype(BF)
                got = to_y(lax.dynamic_slice_in_dim(chip_sum, half_cols * (1 - ypos), half_cols, 2))
                keep = lax.dynamic_slice_in_dim(chip_sum, half_cols * ypos, half_cols, 2)
                done.append((keep.astype(F32) + got.astype(F32)).astype(BF).reshape(own_seqs, rows, heads // 2, HEAD_DIM))
            tables = rot_tables(j * rows, rows)
            k_parts.append(rotary(done[0].astype(F32), tables))
            q_part = rotary(done[1].astype(F32), tables)
            v_parts.append(done[2])
            attn = attend(q_part, jnp.concatenate(k_parts, 1), jnp.concatenate(v_parts, 1), j * rows)
            attn = attn.reshape(own_seqs, rows, half_cols)
            attn_sent.append((attn, to_y(attn)))

        resid = []
        for j in range(CHUNKS):
            attn, got = attn_sent[j]
            both = jnp.concatenate([jnp.where(ypos == 0, attn, got), jnp.where(ypos == 0, got, attn)], -1)
            got = to_core(both)
            rows_all = jnp.concatenate([jnp.where(core == 0, both, got), jnp.where(core == 0, got, both)], 0)
            summed = lax.psum_scatter(dot32(rows_all, w_o).astype(BF), "ty", scatter_dimension=0, tiled=False)
            resid.append((x32[j * rows:(j + 1) * rows] + summed.astype(F32)).astype(BF))

        outs = []
        for j in range(CHUNKS):
            h32 = resid[j].astype(F32)
            n2 = normed(h32, lax.psum(moments(h32), "tx"), full_width)
            n2 = xor_order(n2.reshape(4, quarter, width), me)
            gathered = lax.all_gather(n2, "ty", axis=0)
            away = gathered[:, 1::2]
            far, near = gathered[:, 2], gathered[:, 0]
            sums = []
            for w in (w_gate, w_up):
                got = to_core(dot32(away, w).astype(BF))
                got_y = to_y((dot32(far, w) + got[:, 1].astype(F32)).astype(BF))
                chip_sum = (dot32(near, w) + got[:, 0].astype(F32)).astype(BF)
                sums.append((chip_sum.astype(F32) + got_y.astype(F32)).astype(BF).astype(F32))
            act = (jax.nn.silu(sums[0]) * sums[1]).astype(BF)
            pair = jnp.stack([act, to_y(act)], 1)
            got = to_core(pair)
            act_all = jnp.stack([pair[:, 0], got[:, 0], pair[:, 1], got[:, 1]], 1)
            summed = lax.psum_scatter(dot32(act_all, w_down).astype(BF), "ty", scatter_dimension=0, tiled=False)
            summed = xor_order(summed, me).reshape(rows, width)
            outs.append((h32 + summed.astype(F32)).astype(BF))
        return jnp.concatenate(outs, 0)[None]

    return jax.shard_map(layer_fn, mesh=mesh, in_specs=(act_spec, col_spec, col_spec, col_spec, row_spec, col_spec, col_spec, row_spec), out_specs=act_spec, check_vma=False)
```

```python
import jax
import jax.numpy as jnp
from jax import lax
from jax.experimental import pallas as pl
from jax.experimental.pallas import tpu as pltpu
from jax.sharding import PartitionSpec as P

HEAD_DIM = 128
EPS = 1e-5
THETA = 10000.0
CHUNKS = 2
BF = jnp.bfloat16
F32 = jnp.float32


def rot_tables(start, rows):
    half_dim = HEAD_DIM // 2
    inv_freq = THETA ** (-2.0 * jnp.arange(half_dim, dtype=F32) / HEAD_DIM)
    angles = (start + jnp.arange(rows, dtype=F32))[:, None] * inv_freq[None, :]
    cos_t, sin_t = jnp.cos(angles), jnp.sin(angles)
    return jnp.concatenate([cos_t, cos_t], -1), jnp.concatenate([-sin_t, sin_t], -1)


def rotary(vals, tables):
    cos_t, sin_t = tables
    swapped = jnp.concatenate([vals[..., HEAD_DIM // 2:], vals[..., :HEAD_DIM // 2]], axis=-1)
    return (vals * cos_t[:, None, :] + swapped * sin_t[:, None, :]).astype(BF)


def attend(q, k, v, start):
    rows, keys = q.shape[1], k.shape[1]
    scores = jnp.einsum("nqhd,nkhd->nhqk", q, k, preferred_element_type=F32) * HEAD_DIM ** -0.5
    allowed = (start + jnp.arange(rows))[:, None] >= jnp.arange(keys)[None, :]
    scores = jnp.where(allowed, scores, -1e30)
    prob = jax.nn.softmax(scores, axis=-1).astype(BF)
    return jnp.einsum("nhqk,nkhd->nqhd", prob, v, preferred_element_type=F32).astype(BF)


def dot32(rows, weight):
    return jnp.einsum("...c,ch->...h", rows, weight, preferred_element_type=F32)


def moments(vals):
    return jnp.stack([jnp.sum(vals, axis=-1), jnp.sum(vals * vals, axis=-1)], axis=-1)


def normed(vals, sums, full_width):
    mean_val = sums[..., 0:1] / full_width
    var_val = sums[..., 1:2] / full_width - mean_val * mean_val
    return ((vals - mean_val) * lax.rsqrt(var_val + EPS)).astype(BF)


def xor_order(parts, me):
    parts = jnp.where(me % 2 == 1, jnp.stack([parts[1], parts[0], parts[3], parts[2]]), parts)
    return jnp.where(me >= 2, jnp.stack([parts[2], parts[3], parts[0], parts[1]]), parts)


MESH = pl.DeviceIdType.MESH
TILE = 384
VMEM_LIMIT = 67043328


def flip(index, by):
    low, high = index % 2, index // 2
    by_low, by_high = by % 2, by // 2
    return low + by_low - 2 * low * by_low + 2 * (high + by_high - 2 * high * by_high)


def greet(z, me):
    barrier = pltpu.get_barrier_semaphore()
    for by in (1, 2, 3):
        pl.semaphore_signal(barrier, inc=1, device_id={"ty": flip(z, by)}, device_id_type=MESH)
    pl.semaphore_signal(barrier, inc=1, device_id={"tx": flip(me, 1)}, device_id_type=MESH)
    pl.semaphore_signal(barrier, inc=1, device_id={"tx": flip(me, 2)}, device_id_type=MESH)
    pl.semaphore_wait(barrier, 5)


def remote(src, dst, send_sem, recv_sem, device_id):
    return pltpu.make_async_remote_copy(src_ref=src, dst_ref=dst, send_sem=send_sem, recv_sem=recv_sem, device_id=device_id, device_id_type=MESH)


def mlp_kernel(n2_ref, h_ref, wg_hbm, wu_hbm, wd_hbm, out_ref, xall, w_in, w_out, pbuf, r1, sbuf, r2, abuf, zsend, zrecv, own,
               w_sem, own_sem, az_send, az_recv, p_send, p_recv, ry_send, ry_recv, ay_send, ay_recv, ac_send, ac_recv, zr_send, zr_recv):
    z, me = lax.axis_index("ty"), lax.axis_index("tx")
    core, ypos = me % 2, me // 2
    core_peer, y_peer = {"tx": flip(me, 1)}, {"tx": flip(me, 2)}
    halves, rows, width = n2_ref.shape
    ff = wg_hbm.shape[1]
    tiles = ff // TILE
    all_tiles = 2 * tiles
    quarter = rows // 4
    steps = 4 * halves

    def slot(i):
        return ((i + 1) // 2) % 4, (i + 1) % 2

    def gather_copy(by, half):
        return remote(n2_ref.at[half], xall.at[by, half], az_send.at[by, half], az_recv.at[by, half], {"ty": flip(z, by)})

    def core_copy(i, part):
        group = pl.ds(part * tiles, tiles)
        return remote(pbuf.at[1 - core, group], r1.at[i % 2, group], p_send.at[i % 2, part], p_recv.at[i % 2, part], core_peer)

    def y_copy(i, part):
        group = pl.ds(part * tiles, tiles)
        return remote(sbuf.at[i % 2, 1 - ypos, group], r2.at[i % 3, group], ry_send.at[i % 3, part], ry_recv.at[i % 3, part], y_peer)

    def act_y_copy(i):
        piece = abuf.at[i % 3, core, ypos]
        return remote(piece, piece, ay_send.at[i % 3], ay_recv.at[i % 3], y_peer)

    def act_core_copy(i):
        piece = abuf.at[i % 3, core]
        return remote(piece, piece, ac_send.at[i % 3], ac_recv.at[i % 3], core_peer)

    def scatter_copy(i):
        by, half = slot(i)
        return remote(zsend.at[i % 2], zrecv.at[by - 1, half], zr_send.at[i % 2], zr_recv.at[by - 1, half], {"ty": flip(z, by)})

    loads = [
        pltpu.make_async_copy(wg_hbm, w_in.at[:, pl.ds(0, ff)], w_sem.at[0]),
        pltpu.make_async_copy(wu_hbm, w_in.at[:, pl.ds(ff, ff)], w_sem.at[1]),
        pltpu.make_async_copy(wd_hbm, w_out, w_sem.at[2]),
    ]
    own_copy = pltpu.make_async_copy(n2_ref, xall.at[0], own_sem)
    own_copy.start()
    for load in loads:
        load.start()
    greet(z, me)
    for by in (1, 2, 3):
        for half in range(halves):
            gather_copy(by, half).start()
    own_copy.wait()
    loads[0].wait()
    loads[1].wait()

    def step(i, carry):
        @pl.when(i < steps)
        def _():
            by, half = slot(i)

            @pl.when((i > 0) & (i < steps - 1))
            def _():
                gather_copy(by, half).wait_recv()

            def product(t, carry):
                cols = pl.ds(pl.multiple_of(t * 2 * TILE, 2 * TILE), 2 * TILE)
                part = jnp.dot(xall[by, half], w_in[:, cols], preferred_element_type=F32).astype(BF)
                pbuf[:, 2 * t] = part[:, :TILE].reshape(2, 2, quarter, TILE)
                pbuf[:, 2 * t + 1] = part[:, TILE:].reshape(2, 2, quarter, TILE)
                return carry

            first = (tiles + 1) // 2
            lax.fori_loop(0, first, product, 0)
            core_copy(i, 0).start()
            lax.fori_loop(first, tiles, product, 0)
            core_copy(i, 1).start()
            for part in range(2):
                core_copy(i, part).wait_recv()

                def add(t, carry):
                    total = pbuf[core, t].astype(F32) + r1[i % 2, t].astype(F32)
                    total = total.astype(BF)
                    sbuf[i % 2, 0, t] = total[0]
                    sbuf[i % 2, 1, t] = total[1]
                    return carry

                lax.fori_loop(part * tiles, (part + 1) * tiles, add, 0)
                y_copy(i, part).start()
            for part in range(2):
                core_copy(i, part).wait_send()

        @pl.when((i >= 1) & (i <= steps))
        def _():
            j = i - 1
            for part in range(2):
                y_copy(j, part).wait()

            def gate(t, carry):
                g = (sbuf[j % 2, ypos, t].astype(F32) + r2[j % 3, t].astype(F32)).astype(BF).astype(F32)
                u = (sbuf[j % 2, ypos, tiles + t].astype(F32) + r2[j % 3, tiles + t].astype(F32)).astype(BF).astype(F32)
                cols = pl.ds(pl.multiple_of(t * TILE, TILE), TILE)
                abuf[j % 3, core, ypos, :, cols] = (g * jax.nn.sigmoid(g) * u).astype(BF)
                return carry

            lax.fori_loop(0, tiles, gate, 0)
            act_y_copy(j).start()

        @pl.when(i >= 2)
        def _():
            j = i - 2
            by, half = slot(j)
            act_y_copy(j).wait()
            act_core_copy(j).start()

            @pl.when(j == 0)
            def _():
                loads[2].wait()

            @pl.when((j >= 3) & (j < steps - 1))
            def _():
                scatter_copy(j - 2).wait_send()

            act_core_copy(j).wait()

            def down(t, carry):
                cols = pl.ds(pl.multiple_of(t * 256, 256), 256)
                part = jnp.dot(abuf[j % 3].reshape(rows, ff), w_out[:, cols], preferred_element_type=F32)

                @pl.when(by == 0)
                def _():
                    own[half, :, cols] = part

                @pl.when(by > 0)
                def _():
                    zsend[j % 2, :, cols] = part.astype(BF)
                return carry

            lax.fori_loop(0, width // 256, down, 0)

            @pl.when(by > 0)
            def _():
                scatter_copy(j).start()
        return carry

    lax.fori_loop(0, steps + 2, step, 0)

    for j in (steps - 3, steps - 2):
        scatter_copy(j).wait_send()
    for half in range(halves):
        for by in (1, 2, 3):
            gather_copy(by, half).wait_send()
            remote(zsend.at[0], zrecv.at[by - 1, half], zr_send.at[0], zr_recv.at[by - 1, half], {"ty": flip(z, by)}).wait_recv()

        def finish(t, carry):
            part = pl.ds(pl.multiple_of(t * 32, 32), 32)
            total = own[half, part]
            for by in range(3):
                total += zrecv[by, half, part].astype(F32)
            out_ref[half, part] = (h_ref[half, part].astype(F32) + total.astype(BF).astype(F32)).astype(BF)
            return carry

        lax.fori_loop(0, rows // 32, finish, 0)


def mlp(n2, h, w_gate, w_up, w_down):
    seq_len, width = n2.shape
    ff = w_gate.shape[1]
    halves = 2
    rows = seq_len // halves
    quarter = rows // 4
    tiles = ff // TILE
    dma, vmem = pltpu.SemaphoreType.DMA, pltpu.VMEM
    in_vmem, anywhere = pl.BlockSpec(memory_space=pltpu.VMEM), pl.BlockSpec(memory_space=pl.ANY)
    out = pl.pallas_call(
        mlp_kernel,
        name="mlp",
        out_shape=jax.ShapeDtypeStruct((halves, rows, width), BF),
        in_specs=[in_vmem, in_vmem, anywhere, anywhere, anywhere],
        out_specs=in_vmem,
        scratch_shapes=[
            vmem((4, halves, rows, width), BF),
            vmem((width, 2 * ff), BF),
            vmem((ff, width), BF),
            vmem((2, 2 * tiles, 2, quarter, TILE), BF),
            vmem((2, 2 * tiles, 2, quarter, TILE), BF),
            vmem((2, 2, 2 * tiles, quarter, TILE), BF),
            vmem((3, 2 * tiles, quarter, TILE), BF),
            vmem((3, 2, 2, quarter, ff), BF),
            vmem((2, rows, width), BF),
            vmem((3, halves, rows, width), BF),
            vmem((halves, rows, width), F32),
            dma((3,)), dma, dma((4, halves)), dma((4, halves)),
            dma((2, 2)), dma((2, 2)), dma((3, 2)), dma((3, 2)),
            dma((3,)), dma((3,)), dma((3,)), dma((3,)),
            dma((2,)), dma((3, halves)),
        ],
        compiler_params=pltpu.CompilerParams(collective_id=0, has_side_effects=True, vmem_limit_bytes=VMEM_LIMIT),
    )(n2.reshape(halves, rows, width), h.reshape(halves, rows, width), w_gate, w_up, w_down)
    return out.reshape(seq_len, width)


def solution(mesh):
    tx_count = mesh.shape["tx"]
    act_spec = P(("dp", "ty"), None, "tx")
    col_spec = P("tx", "ty")
    row_spec = P("ty", "tx")
    core_pairs = [(i, i ^ 1) for i in range(4)]
    y_pairs = [(i, i ^ 2) for i in range(4)]

    def to_core(val):
        return lax.ppermute(val, "tx", core_pairs)

    def to_y(val):
        return lax.ppermute(val, "tx", y_pairs)

    def layer_fn(x_blk, w_q, w_k, w_v, w_o, w_gate, w_up, w_down):
        me = lax.axis_index("tx")
        core, ypos = me % 2, me // 2
        seq_len, width = x_blk.shape[1:]
        full_width = width * tx_count
        n_seqs = lax.axis_size("ty")
        own_seqs = n_seqs // 2
        rows = seq_len // CHUNKS
        quarter = rows // 4
        heads = w_q.shape[1] // HEAD_DIM
        half_cols = w_q.shape[1] // 2
        x32 = x_blk[0].astype(F32)
        n1 = normed(x32, lax.psum(moments(x32), "tx"), full_width)

        k_parts, v_parts, attn_sent = [], [], []
        for j in range(CHUNKS):
            gathered = lax.all_gather(n1[j * rows:(j + 1) * rows], "ty", axis=0)
            mine = lax.dynamic_slice_in_dim(gathered, own_seqs * core, own_seqs, 0)
            other = lax.dynamic_slice_in_dim(gathered, own_seqs * (1 - core), own_seqs, 0)
            done = []
            for w in (w_k, w_q, w_v):
                got = to_core(dot32(other, w).astype(BF))
                chip_sum = (dot32(mine, w) + got.astype(F32)).astype(BF)
                got = to_y(lax.dynamic_slice_in_dim(chip_sum, half_cols * (1 - ypos), half_cols, 2))
                keep = lax.dynamic_slice_in_dim(chip_sum, half_cols * ypos, half_cols, 2)
                done.append((keep.astype(F32) + got.astype(F32)).astype(BF).reshape(own_seqs, rows, heads // 2, HEAD_DIM))
            tables = rot_tables(j * rows, rows)
            k_parts.append(rotary(done[0].astype(F32), tables))
            q_part = rotary(done[1].astype(F32), tables)
            v_parts.append(done[2])
            attn = attend(q_part, jnp.concatenate(k_parts, 1), jnp.concatenate(v_parts, 1), j * rows)
            attn = attn.reshape(own_seqs, rows, half_cols)
            attn_sent.append((attn, to_y(attn)))

        resid = []
        for j in range(CHUNKS):
            attn, got = attn_sent[j]
            both = jnp.concatenate([jnp.where(ypos == 0, attn, got), jnp.where(ypos == 0, got, attn)], -1)
            got = to_core(both)
            rows_all = jnp.concatenate([jnp.where(core == 0, both, got), jnp.where(core == 0, got, both)], 0)
            summed = lax.psum_scatter(dot32(rows_all, w_o).astype(BF), "ty", scatter_dimension=0, tiled=False)
            resid.append((x32[j * rows:(j + 1) * rows] + summed.astype(F32)).astype(BF))

        h = jnp.concatenate(resid, 0)
        h32 = h.astype(F32)
        n2 = normed(h32, lax.psum(moments(h32), "tx"), full_width)
        return mlp(n2, h, w_gate, w_up, w_down)[None]

    return jax.shard_map(layer_fn, mesh=mesh, in_specs=(act_spec, col_spec, col_spec, col_spec, row_spec, col_spec, col_spec, row_spec), out_specs=act_spec, check_vma=False)
```

```python
import jax
import jax.numpy as jnp
import numpy as np
from jax import lax
from jax.experimental import pallas as pl
from jax.experimental.pallas import tpu as pltpu
from jax.sharding import PartitionSpec as P

HEAD_DIM = 128
EPS = 1e-5
THETA = 10000.0
BF = jnp.bfloat16
F32 = jnp.float32


def rot_tables(seq_len):
    half_dim = HEAD_DIM // 2
    inv_freq = np.float32(THETA) ** (-2.0 * np.arange(half_dim, dtype=np.float32) / np.float32(HEAD_DIM))
    angles = np.arange(seq_len, dtype=np.float32)[:, None] * inv_freq.astype(np.float32)[None, :]
    cos_t, sin_t = np.cos(angles), np.sin(angles)
    return np.concatenate([cos_t, cos_t], -1), np.concatenate([-sin_t, sin_t], -1)


def moments(vals):
    return jnp.stack([jnp.sum(vals, axis=-1), jnp.sum(vals * vals, axis=-1)], axis=-1)


def normed(vals, sums, full_width):
    mean_val = sums[..., 0:1] / full_width
    var_val = sums[..., 1:2] / full_width - mean_val * mean_val
    return ((vals - mean_val) * lax.rsqrt(var_val + EPS)).astype(BF)


MESH = pl.DeviceIdType.MESH
TILE = 384
VMEM_LIMIT = 67043328


def flip(index, by):
    low, high = index % 2, index // 2
    by_low, by_high = by % 2, by // 2
    return low + by_low - 2 * low * by_low + 2 * (high + by_high - 2 * high * by_high)


def greet(z, me):
    barrier = pltpu.get_barrier_semaphore()
    for by in (1, 2, 3):
        pl.semaphore_signal(barrier, inc=1, device_id={"ty": flip(z, by)}, device_id_type=MESH)
    pl.semaphore_signal(barrier, inc=1, device_id={"tx": flip(me, 1)}, device_id_type=MESH)
    pl.semaphore_signal(barrier, inc=1, device_id={"tx": flip(me, 2)}, device_id_type=MESH)
    pl.semaphore_wait(barrier, 5)


def remote(src, dst, send_sem, recv_sem, device_id):
    return pltpu.make_async_remote_copy(src_ref=src, dst_ref=dst, send_sem=send_sem, recv_sem=recv_sem, device_id=device_id, device_id_type=MESH)


def attn_kernel(n1_ref, x_ref, cos_ref, sin_ref, wq_hbm, wk_hbm, wv_hbm, wo_hbm, out_ref, xall, w_in, w_out, pbuf, r1, sbuf, r2, qbuf, kvbuf, abuf, zsend, zrecv, own,
                w_sem, own_sem, az_send, az_recv, p_send, p_recv, ry_send, ry_recv, kv_send, kv_recv, ay_send, ay_recv, ac_send, ac_recv, zr_send, zr_recv):
    z, me = lax.axis_index("ty"), lax.axis_index("tx")
    core, ypos = me % 2, me // 2
    core_peer, y_peer = {"tx": flip(me, 1)}, {"tx": flip(me, 2)}
    _, rows, width = n1_ref.shape
    half_cols = width // 2
    heads = half_cols // HEAD_DIM
    steps = 4
    inner = flip(z % 2, z // 2)

    def slot(i):
        turn = (i + 1) % 4
        return inner * ((4 - turn) % 4) + (1 - inner) * turn

    right_slot, left_slot = 1 + 2 * (z % 2), 3 - 2 * (z % 2)
    to_right = remote(n1_ref, xall.at[right_slot], az_send.at[0], az_recv.at[right_slot], {"ty": (z + 1) % 4})
    to_left = remote(n1_ref, xall.at[left_slot], az_send.at[1], az_recv.at[left_slot], {"ty": (z + 3) % 4})
    on_right = remote(xall.at[left_slot], xall.at[2], az_send.at[2], az_recv.at[2], {"ty": (z + 1) % 4})
    on_left = remote(xall.at[right_slot], xall.at[2], az_send.at[3], az_recv.at[2], {"ty": (z + 3) % 4})
    to_end = remote(xall.at[2], xall.at[3], az_send.at[4], az_recv.at[3], {"ty": (3 * z + 1) % 4})

    def arrived(by):
        remote(xall.at[by], xall.at[by], az_send.at[0], az_recv.at[by], {"ty": flip(z, 1)}).wait_recv()

    def core_copy(i):
        return remote(pbuf.at[1 - core], r1.at[i % 2], p_send.at[i % 2], p_recv.at[i % 2], core_peer)

    def y_copy(i):
        return remote(sbuf.at[i % 2, 1 - ypos], r2.at[i % 3], ry_send.at[i % 3], ry_recv.at[i % 3], y_peer)

    def kv_copy(i):
        piece = kvbuf.at[i % 2, core]
        return remote(piece, piece, kv_send.at[i % 2], kv_recv.at[i % 2], core_peer)

    def out_y_copy(i):
        piece = abuf.at[i % 3, core, ypos]
        return remote(piece, piece, ay_send.at[i % 3], ay_recv.at[i % 3], y_peer)

    def out_core_copy(i):
        piece = abuf.at[i % 3, core]
        return remote(piece, piece, ac_send.at[i % 3], ac_recv.at[i % 3], core_peer)

    def scatter_copy(i):
        by = slot(i)
        return remote(zsend.at[i % 2], zrecv.at[by - 1], zr_send.at[i % 2], zr_recv.at[by - 1], {"ty": flip(z, by)})

    loads = [pltpu.make_async_copy(w, w_in.at[n], w_sem.at[n]) for n, w in enumerate((wq_hbm, wk_hbm, wv_hbm))]
    loads.append(pltpu.make_async_copy(wo_hbm, w_out, w_sem.at[3]))
    own_copy = pltpu.make_async_copy(n1_ref, xall.at[0], own_sem)
    greet(z, me)

    @pl.when(z < 3)
    def _():
        to_right.start()

    @pl.when(z > 0)
    def _():
        to_left.start()

    own_copy.start()
    for load in loads:
        load.start()
    own_copy.wait()
    for load in loads:
        load.wait()

    @pl.when(z > 0)
    def _():
        arrived(left_slot)

    @pl.when((z > 0) & (z < 3))
    def _():
        on_right.start()

    @pl.when(z < 3)
    def _():
        arrived(right_slot)

    @pl.when((z > 0) & (z < 3))
    def _():
        on_left.start()

    def step(i, carry):
        @pl.when(i < steps)
        def _():
            by = slot(i)

            @pl.when(i == 1)
            def _():
                arrived(2)

                @pl.when((z > 0) & (z < 3))
                def _():
                    to_end.start()

            @pl.when((i == 2) & (z != 1) & (z != 2))
            def _():
                arrived(3)

            def product(t, carry):
                part = jnp.dot(xall[by, 1 - core], w_in[t], preferred_element_type=F32).astype(BF)
                pbuf[1 - core, 0, t] = part[:, :half_cols]
                pbuf[1 - core, 1, t] = part[:, half_cols:]
                return carry

            def near(t, carry):
                part = jnp.dot(xall[by, core], w_in[t], preferred_element_type=F32).astype(BF)
                pbuf[core, 0, t] = part[:, :half_cols]
                pbuf[core, 1, t] = part[:, half_cols:]
                return carry

            lax.fori_loop(0, 3, product, 0)
            core_copy(i).start()
            lax.fori_loop(0, 3, near, 0)
            core_copy(i).wait()

            def add(t, carry):
                for side in range(2):
                    sbuf[i % 2, side, t] = (pbuf[core, side, t].astype(F32) + r1[i % 2, side, t].astype(F32)).astype(BF)
                return carry

            lax.fori_loop(0, 3, add, 0)
            y_copy(i).start()

        @pl.when((i >= 1) & (i <= steps))
        def _():
            j = i - 1
            y_copy(j).wait()
            for h in range(heads):
                cols = slice(h * HEAD_DIM, (h + 1) * HEAD_DIM)

                def total(n):
                    return (sbuf[j % 2, ypos, n, :, cols].astype(F32) + r2[j % 3, n, :, cols].astype(F32)).astype(BF)

                def turned(vals):
                    vals = vals.astype(F32)
                    return (vals * cos_ref[core] + pltpu.roll(vals, HEAD_DIM // 2, 1) * sin_ref[core]).astype(BF)

                qbuf[:, cols] = turned(total(0))
                kvbuf[j % 2, core, 0, :, cols] = turned(total(1))
                kvbuf[j % 2, core, 1, :, cols] = total(2)
            kv_copy(j).start()
            kv_copy(j).wait()
            q_pos = core * rows + lax.broadcasted_iota(jnp.int32, (rows, 2 * rows), 0)
            allowed = q_pos >= lax.broadcasted_iota(jnp.int32, (rows, 2 * rows), 1)
            for h in range(heads):
                cols = slice(h * HEAD_DIM, (h + 1) * HEAD_DIM)
                keys = kvbuf[j % 2, :, 0, :, cols].reshape(2 * rows, HEAD_DIM)
                vals = kvbuf[j % 2, :, 1, :, cols].reshape(2 * rows, HEAD_DIM)
                scores = lax.dot_general(qbuf[:, cols], keys, (((1,), (1,)), ((), ())), preferred_element_type=F32) * HEAD_DIM ** -0.5
                scores = jnp.where(allowed, scores, -1e30)
                weight = jnp.exp(scores - jnp.max(scores, axis=1, keepdims=True))
                prob = (weight / jnp.sum(weight, axis=1, keepdims=True)).astype(BF)
                abuf[j % 3, core, ypos, :, cols] = jnp.dot(prob, vals, preferred_element_type=F32).astype(BF)
            out_y_copy(j).start()

        @pl.when(i >= 2)
        def _():
            j = i - 2
            by = slot(j)
            out_y_copy(j).wait()
            out_core_copy(j).start()

            @pl.when((j >= 2) & (j < steps - 1))
            def _():
                scatter_copy(j - 2).wait_send()

            out_core_copy(j).wait()

            def out(t, carry):
                cols = pl.ds(pl.multiple_of(t * 256, 256), 256)
                for half in range(2):
                    part = jnp.dot(abuf[j % 3, half, 0], w_out[0:half_cols, cols], preferred_element_type=F32)
                    part += jnp.dot(abuf[j % 3, half, 1], w_out[half_cols:, cols], preferred_element_type=F32)

                    @pl.when(by == 0)
                    def _():
                        own[half, :, cols] = part

                    @pl.when(by > 0)
                    def _():
                        zsend[j % 2, half, :, cols] = part.astype(BF)
                return carry

            lax.fori_loop(0, width // 256, out, 0)

            @pl.when(by > 0)
            def _():
                scatter_copy(j).start()
        return carry

    lax.fori_loop(0, steps + 2, step, 0)

    @pl.when(z < 3)
    def _():
        to_right.wait_send()

    @pl.when(z > 0)
    def _():
        to_left.wait_send()

    @pl.when((z > 0) & (z < 3))
    def _():
        on_right.wait_send()
        on_left.wait_send()
        to_end.wait_send()

    for j in (steps - 3, steps - 2):
        scatter_copy(j).wait_send()
    for by in (1, 2, 3):
        remote(zsend.at[0], zrecv.at[by - 1], zr_send.at[0], zr_recv.at[by - 1], {"ty": flip(z, by)}).wait_recv()

    def finish(t, carry):
        part = pl.ds(pl.multiple_of(t * 32, 32), 32)
        for half in range(2):
            total = own[half, part]
            for by in range(3):
                total += zrecv[by, half, part].astype(F32)
            out_ref[half, part] = (x_ref[half, part].astype(F32) + total.astype(BF).astype(F32)).astype(BF)
        return carry

    lax.fori_loop(0, rows // 32, finish, 0)


def attention(n1, x, w_q, w_k, w_v, w_o):
    seq_len, width = n1.shape
    rows, half_cols = seq_len // 2, width // 2
    cos_t, sin_t = rot_tables(seq_len)
    dma, vmem = pltpu.SemaphoreType.DMA, pltpu.VMEM
    in_vmem, anywhere = pl.BlockSpec(memory_space=pltpu.VMEM), pl.BlockSpec(memory_space=pl.ANY)
    out = pl.pallas_call(
        attn_kernel,
        name="attention",
        out_shape=jax.ShapeDtypeStruct((2, rows, width), BF),
        in_specs=[in_vmem] * 4 + [anywhere] * 4,
        out_specs=in_vmem,
        scratch_shapes=[
            vmem((4, 2, rows, width), BF),
            vmem((3, width, width), BF),
            vmem((width, width), BF),
            vmem((2, 2, 3, rows, half_cols), BF),
            vmem((2, 2, 3, rows, half_cols), BF),
            vmem((2, 2, 3, rows, half_cols), BF),
            vmem((3, 3, rows, half_cols), BF),
            vmem((rows, half_cols), BF),
            vmem((2, 2, 2, rows, half_cols), BF),
            vmem((3, 2, 2, rows, half_cols), BF),
            vmem((2, 2, rows, width), BF),
            vmem((3, 2, rows, width), BF),
            vmem((2, rows, width), F32),
            dma((4,)), dma, dma((5,)), dma((4,)),
            dma((2,)), dma((2,)), dma((3,)), dma((3,)), dma((2,)), dma((2,)),
            dma((3,)), dma((3,)), dma((3,)), dma((3,)),
            dma((2,)), dma((3,)),
        ],
        compiler_params=pltpu.CompilerParams(collective_id=1, has_side_effects=True, vmem_limit_bytes=VMEM_LIMIT),
    )(n1.reshape(2, rows, width), x.reshape(2, rows, width), jnp.asarray(cos_t).reshape(2, rows, HEAD_DIM), jnp.asarray(sin_t).reshape(2, rows, HEAD_DIM), w_q, w_k, w_v, w_o)
    return out.reshape(seq_len, width)


def mlp_kernel(n2_ref, h_ref, wg_hbm, wu_hbm, wd_hbm, out_ref, xall, w_in, w_out, pbuf, r1, sbuf, r2, abuf, zsend, zrecv, own,
               w_sem, own_sem, az_send, az_recv, p_send, p_recv, ry_send, ry_recv, ay_send, ay_recv, ac_send, ac_recv, zr_send, zr_recv):
    z, me = lax.axis_index("ty"), lax.axis_index("tx")
    core, ypos = me % 2, me // 2
    core_peer, y_peer = {"tx": flip(me, 1)}, {"tx": flip(me, 2)}
    halves, rows, width = n2_ref.shape
    ff = wg_hbm.shape[1]
    tiles = ff // TILE
    all_tiles = 2 * tiles
    quarter = rows // 4
    steps = 4 * halves

    def slot(i):
        return ((i + 1) // 2) % 4, (i + 1) % 2

    def gather_copy(by, half):
        return remote(n2_ref.at[half], xall.at[by, half], az_send.at[by, half], az_recv.at[by, half], {"ty": flip(z, by)})

    def core_copy(i, part):
        group = pl.ds(part * tiles, tiles)
        return remote(pbuf.at[1 - core, group], r1.at[i % 2, group], p_send.at[i % 2, part], p_recv.at[i % 2, part], core_peer)

    def y_copy(i, part):
        group = pl.ds(part * tiles, tiles)
        return remote(sbuf.at[i % 2, 1 - ypos, group], r2.at[i % 3, group], ry_send.at[i % 3, part], ry_recv.at[i % 3, part], y_peer)

    def act_y_copy(i):
        piece = abuf.at[i % 3, core, ypos]
        return remote(piece, piece, ay_send.at[i % 3], ay_recv.at[i % 3], y_peer)

    def act_core_copy(i):
        piece = abuf.at[i % 3, core]
        return remote(piece, piece, ac_send.at[i % 3], ac_recv.at[i % 3], core_peer)

    def scatter_copy(i):
        by, half = slot(i)
        return remote(zsend.at[i % 2], zrecv.at[by - 1, half], zr_send.at[i % 2], zr_recv.at[by - 1, half], {"ty": flip(z, by)})

    loads = [
        pltpu.make_async_copy(wg_hbm, w_in.at[:, pl.ds(0, ff)], w_sem.at[0]),
        pltpu.make_async_copy(wu_hbm, w_in.at[:, pl.ds(ff, ff)], w_sem.at[1]),
        pltpu.make_async_copy(wd_hbm, w_out, w_sem.at[2]),
    ]
    own_copy = pltpu.make_async_copy(n2_ref, xall.at[0], own_sem)
    own_copy.start()
    for load in loads:
        load.start()
    greet(z, me)
    for by in (1, 2, 3):
        for half in range(halves):
            gather_copy(by, half).start()
    own_copy.wait()
    loads[0].wait()
    loads[1].wait()

    def step(i, carry):
        @pl.when(i < steps)
        def _():
            by, half = slot(i)

            @pl.when((i > 0) & (i < steps - 1))
            def _():
                gather_copy(by, half).wait_recv()

            def product(t, carry):
                cols = pl.ds(pl.multiple_of(t * 2 * TILE, 2 * TILE), 2 * TILE)
                part = jnp.dot(xall[by, half], w_in[:, cols], preferred_element_type=F32).astype(BF)
                pbuf[:, 2 * t] = part[:, :TILE].reshape(2, 2, quarter, TILE)
                pbuf[:, 2 * t + 1] = part[:, TILE:].reshape(2, 2, quarter, TILE)
                return carry

            first = (tiles + 1) // 2
            lax.fori_loop(0, first, product, 0)
            core_copy(i, 0).start()
            lax.fori_loop(first, tiles, product, 0)
            core_copy(i, 1).start()
            for part in range(2):
                core_copy(i, part).wait_recv()

                def add(t, carry):
                    total = pbuf[core, t].astype(F32) + r1[i % 2, t].astype(F32)
                    total = total.astype(BF)
                    sbuf[i % 2, 0, t] = total[0]
                    sbuf[i % 2, 1, t] = total[1]
                    return carry

                lax.fori_loop(part * tiles, (part + 1) * tiles, add, 0)
                y_copy(i, part).start()
            for part in range(2):
                core_copy(i, part).wait_send()

        @pl.when((i >= 1) & (i <= steps))
        def _():
            j = i - 1
            for part in range(2):
                y_copy(j, part).wait()

            def gate(t, carry):
                g = (sbuf[j % 2, ypos, t].astype(F32) + r2[j % 3, t].astype(F32)).astype(BF).astype(F32)
                u = (sbuf[j % 2, ypos, tiles + t].astype(F32) + r2[j % 3, tiles + t].astype(F32)).astype(BF).astype(F32)
                cols = pl.ds(pl.multiple_of(t * TILE, TILE), TILE)
                abuf[j % 3, core, ypos, :, cols] = (g * jax.nn.sigmoid(g) * u).astype(BF)
                return carry

            lax.fori_loop(0, tiles, gate, 0)
            act_y_copy(j).start()

        @pl.when(i >= 2)
        def _():
            j = i - 2
            by, half = slot(j)
            act_y_copy(j).wait()
            act_core_copy(j).start()

            @pl.when(j == 0)
            def _():
                loads[2].wait()

            @pl.when((j >= 3) & (j < steps - 1))
            def _():
                scatter_copy(j - 2).wait_send()

            act_core_copy(j).wait()

            def down(t, carry):
                cols = pl.ds(pl.multiple_of(t * 256, 256), 256)
                part = jnp.dot(abuf[j % 3].reshape(rows, ff), w_out[:, cols], preferred_element_type=F32)

                @pl.when(by == 0)
                def _():
                    own[half, :, cols] = part

                @pl.when(by > 0)
                def _():
                    zsend[j % 2, :, cols] = part.astype(BF)
                return carry

            lax.fori_loop(0, width // 256, down, 0)

            @pl.when(by > 0)
            def _():
                scatter_copy(j).start()
        return carry

    lax.fori_loop(0, steps + 2, step, 0)

    for j in (steps - 3, steps - 2):
        scatter_copy(j).wait_send()
    for half in range(halves):
        for by in (1, 2, 3):
            gather_copy(by, half).wait_send()
            remote(zsend.at[0], zrecv.at[by - 1, half], zr_send.at[0], zr_recv.at[by - 1, half], {"ty": flip(z, by)}).wait_recv()

        def finish(t, carry):
            part = pl.ds(pl.multiple_of(t * 32, 32), 32)
            total = own[half, part]
            for by in range(3):
                total += zrecv[by, half, part].astype(F32)
            out_ref[half, part] = (h_ref[half, part].astype(F32) + total.astype(BF).astype(F32)).astype(BF)
            return carry

        lax.fori_loop(0, rows // 32, finish, 0)


def mlp(n2, h, w_gate, w_up, w_down):
    seq_len, width = n2.shape
    ff = w_gate.shape[1]
    halves = 2
    rows = seq_len // halves
    quarter = rows // 4
    tiles = ff // TILE
    dma, vmem = pltpu.SemaphoreType.DMA, pltpu.VMEM
    in_vmem, anywhere = pl.BlockSpec(memory_space=pltpu.VMEM), pl.BlockSpec(memory_space=pl.ANY)
    out = pl.pallas_call(
        mlp_kernel,
        name="mlp",
        out_shape=jax.ShapeDtypeStruct((halves, rows, width), BF),
        in_specs=[in_vmem, in_vmem, anywhere, anywhere, anywhere],
        out_specs=in_vmem,
        scratch_shapes=[
            vmem((4, halves, rows, width), BF),
            vmem((width, 2 * ff), BF),
            vmem((ff, width), BF),
            vmem((2, 2 * tiles, 2, quarter, TILE), BF),
            vmem((2, 2 * tiles, 2, quarter, TILE), BF),
            vmem((2, 2, 2 * tiles, quarter, TILE), BF),
            vmem((3, 2 * tiles, quarter, TILE), BF),
            vmem((3, 2, 2, quarter, ff), BF),
            vmem((2, rows, width), BF),
            vmem((3, halves, rows, width), BF),
            vmem((halves, rows, width), F32),
            dma((3,)), dma, dma((4, halves)), dma((4, halves)),
            dma((2, 2)), dma((2, 2)), dma((3, 2)), dma((3, 2)),
            dma((3,)), dma((3,)), dma((3,)), dma((3,)),
            dma((2,)), dma((3, halves)),
        ],
        compiler_params=pltpu.CompilerParams(collective_id=0, has_side_effects=True, vmem_limit_bytes=VMEM_LIMIT),
    )(n2.reshape(halves, rows, width), h.reshape(halves, rows, width), w_gate, w_up, w_down)
    return out.reshape(seq_len, width)


def solution(mesh):
    tx_count = mesh.shape["tx"]
    act_spec = P(("dp", "ty"), None, "tx")
    col_spec = P("tx", "ty")
    row_spec = P("ty", "tx")

    def layer_fn(x_blk, w_q, w_k, w_v, w_o, w_gate, w_up, w_down):
        full_width = x_blk.shape[-1] * tx_count

        def norm(vals):
            vals = vals.astype(F32)
            return normed(vals, lax.psum(moments(vals), "tx"), full_width)

        x = x_blk[0]
        h = attention(norm(x), x, w_q, w_k, w_v, w_o)
        return mlp(norm(h), h, w_gate, w_up, w_down)[None]

    return jax.shard_map(layer_fn, mesh=mesh, in_specs=(act_spec, col_spec, col_spec, col_spec, row_spec, col_spec, col_spec, row_spec), out_specs=act_spec, check_vma=False)
```

```python
import jax
import jax.numpy as jnp
import numpy as np
from jax import lax
from jax.experimental import pallas as pl
from jax.experimental.pallas import tpu as pltpu
from jax.sharding import PartitionSpec as P

HEAD_DIM = 128
EPS = 1e-5
THETA = 10000.0
BF = jnp.bfloat16
F32 = jnp.float32


def rot_tables(seq_len):
    half_dim = HEAD_DIM // 2
    inv_freq = np.float32(THETA) ** (-2.0 * np.arange(half_dim, dtype=np.float32) / np.float32(HEAD_DIM))
    angles = np.arange(seq_len, dtype=np.float32)[:, None] * inv_freq.astype(np.float32)[None, :]
    cos_t, sin_t = np.cos(angles), np.sin(angles)
    return np.concatenate([cos_t, cos_t], -1), np.concatenate([-sin_t, sin_t], -1)


MESH = pl.DeviceIdType.MESH
TILE = 384
VMEM_LIMIT = 67043328


def flip(index, by):
    low, high = index % 2, index // 2
    by_low, by_high = by % 2, by // 2
    return low + by_low - 2 * low * by_low + 2 * (high + by_high - 2 * high * by_high)


def greet(z, me):
    barrier = pltpu.get_barrier_semaphore()
    for by in (1, 2, 3):
        pl.semaphore_signal(barrier, inc=1, device_id={"ty": flip(z, by)}, device_id_type=MESH)
    pl.semaphore_signal(barrier, inc=1, device_id={"tx": flip(me, 1)}, device_id_type=MESH)
    pl.semaphore_signal(barrier, inc=1, device_id={"tx": flip(me, 2)}, device_id_type=MESH)
    pl.semaphore_wait(barrier, 5)


def norm_rows(src, dst, stats, send_sem, recv_sem, core_peer, y_peer):
    halves, rows, width = src.shape
    total_rows = halves * rows
    full_width = 4 * width
    lane = lax.broadcasted_iota(jnp.int32, (rows, 128), 1)
    for half in range(halves):
        vals = src[half].astype(F32)
        both = jnp.where(lane == 0, jnp.sum(vals, axis=1, keepdims=True), jnp.sum(vals * vals, axis=1, keepdims=True))
        stats[0, :, half * rows:(half + 1) * rows] = both.T[:8]
    swap = remote(stats.at[0], stats.at[1], send_sem.at[0], recv_sem.at[0], core_peer)
    swap.start()
    swap.wait()
    stats[2] = stats[0] + stats[1]
    swap = remote(stats.at[2], stats.at[3], send_sem.at[1], recv_sem.at[1], y_peer)
    swap.start()
    swap.wait()
    sums = stats[2] + stats[3]
    sums = jnp.concatenate([sums, jnp.zeros((120, total_rows), F32)], 0).T
    mean_val = sums[:, 0:1] / full_width
    var_val = sums[:, 1:2] / full_width - mean_val * mean_val
    scale = lax.rsqrt(var_val + EPS)
    for half in range(halves):
        part = slice(half * rows, (half + 1) * rows)
        dst[half] = ((src[half].astype(F32) - mean_val[part]) * scale[part]).astype(BF)


def remote(src, dst, send_sem, recv_sem, device_id):
    return pltpu.make_async_remote_copy(src_ref=src, dst_ref=dst, send_sem=send_sem, recv_sem=recv_sem, device_id=device_id, device_id_type=MESH)


def attn_kernel(x_ref, cos_ref, sin_ref, wq_hbm, wk_hbm, wv_hbm, wo_hbm, out_ref, xall, w_in, w_out, pbuf, r1, sbuf, r2, qbuf, kvbuf, abuf, zsend, zrecv, own,
                stats, s_send, s_recv, w_sem, az_send, az_recv, p_send, p_recv, ry_send, ry_recv, kv_send, kv_recv, ay_send, ay_recv, ac_send, ac_recv, zr_send, zr_recv):
    z, me = lax.axis_index("ty"), lax.axis_index("tx")
    core, ypos = me % 2, me // 2
    core_peer, y_peer = {"tx": flip(me, 1)}, {"tx": flip(me, 2)}
    _, rows, width = x_ref.shape
    half_cols = width // 2
    heads = half_cols // HEAD_DIM
    steps = 4
    inner = flip(z % 2, z // 2)

    def slot(i):
        return inner * ((4 - i) % 4) + (1 - inner) * (i % 4)

    right_slot, left_slot = 1 + 2 * (z % 2), 3 - 2 * (z % 2)
    to_right = remote(xall.at[0], xall.at[right_slot], az_send.at[0], az_recv.at[right_slot], {"ty": (z + 1) % 4})
    to_left = remote(xall.at[0], xall.at[left_slot], az_send.at[1], az_recv.at[left_slot], {"ty": (z + 3) % 4})
    on_right = remote(xall.at[left_slot], xall.at[2], az_send.at[2], az_recv.at[2], {"ty": (z + 1) % 4})
    on_left = remote(xall.at[right_slot], xall.at[2], az_send.at[3], az_recv.at[2], {"ty": (z + 3) % 4})
    to_end = remote(xall.at[2], xall.at[3], az_send.at[4], az_recv.at[3], {"ty": (3 * z + 1) % 4})

    def arrived(by):
        remote(xall.at[by], xall.at[by], az_send.at[0], az_recv.at[by], {"ty": flip(z, 1)}).wait_recv()

    def core_copy(i):
        return remote(pbuf.at[1 - core], r1.at[i % 2], p_send.at[i % 2], p_recv.at[i % 2], core_peer)

    def y_copy(i):
        return remote(sbuf.at[i % 2, 1 - ypos], r2.at[i % 3], ry_send.at[i % 3], ry_recv.at[i % 3], y_peer)

    def kv_copy(i):
        piece = kvbuf.at[i % 2, core]
        return remote(piece, piece, kv_send.at[i % 2], kv_recv.at[i % 2], core_peer)

    def out_y_copy(i):
        piece = abuf.at[i % 3, core, ypos]
        return remote(piece, piece, ay_send.at[i % 3], ay_recv.at[i % 3], y_peer)

    def out_core_copy(i):
        piece = abuf.at[i % 3, core]
        return remote(piece, piece, ac_send.at[i % 3], ac_recv.at[i % 3], core_peer)

    def scatter_copy(i, half):
        by = slot(i)
        return remote(zsend.at[i % 2, half], zrecv.at[by - 1, half], zr_send.at[i % 2, half], zr_recv.at[by - 1, half], {"ty": flip(z, by)})

    loads = [pltpu.make_async_copy(w, w_in.at[n], w_sem.at[n]) for n, w in enumerate((wq_hbm, wk_hbm, wv_hbm))]
    loads.append(pltpu.make_async_copy(wo_hbm, w_out, w_sem.at[3]))
    for load in loads:
        load.start()
    greet(z, me)
    norm_rows(x_ref, xall.at[0], stats, s_send, s_recv, core_peer, y_peer)

    @pl.when(z < 3)
    def _():
        to_right.start()

    @pl.when(z > 0)
    def _():
        to_left.start()

    for load in loads:
        load.wait()

    def step(i, carry):
        @pl.when(i < steps)
        def _():
            by = slot(i)

            @pl.when((i == 1) & (z > 0))
            def _():
                arrived(left_slot)

            @pl.when((i == 1) & (z > 0) & (z < 3))
            def _():
                on_right.start()

            @pl.when((i == 1) & (z < 3))
            def _():
                arrived(right_slot)

            @pl.when((i == 1) & (z > 0) & (z < 3))
            def _():
                on_left.start()

            @pl.when(i == 2)
            def _():
                arrived(2)

            @pl.when((i == 2) & (z > 0) & (z < 3))
            def _():
                to_end.start()

            @pl.when((i == 3) & (z != 1) & (z != 2))
            def _():
                arrived(3)

            def product(t, carry):
                part = jnp.dot(xall[by, 1 - core], w_in[t], preferred_element_type=F32).astype(BF)
                pbuf[1 - core, 0, t] = part[:, :half_cols]
                pbuf[1 - core, 1, t] = part[:, half_cols:]
                return carry

            def near(t, carry):
                part = jnp.dot(xall[by, core], w_in[t], preferred_element_type=F32).astype(BF)
                pbuf[core, 0, t] = part[:, :half_cols]
                pbuf[core, 1, t] = part[:, half_cols:]
                return carry

            lax.fori_loop(0, 3, product, 0)
            core_copy(i).start()
            lax.fori_loop(0, 3, near, 0)
            core_copy(i).wait()

            def add(t, carry):
                for side in range(2):
                    sbuf[i % 2, side, t] = (pbuf[core, side, t].astype(F32) + r1[i % 2, side, t].astype(F32)).astype(BF)
                return carry

            lax.fori_loop(0, 3, add, 0)
            y_copy(i).start()

        @pl.when((i >= 1) & (i <= steps))
        def _():
            j = i - 1
            y_copy(j).wait()
            for h in range(heads):
                cols = slice(h * HEAD_DIM, (h + 1) * HEAD_DIM)

                def total(n):
                    return (sbuf[j % 2, ypos, n, :, cols].astype(F32) + r2[j % 3, n, :, cols].astype(F32)).astype(BF)

                def turned(vals):
                    vals = vals.astype(F32)
                    return (vals * cos_ref[core] + pltpu.roll(vals, HEAD_DIM // 2, 1) * sin_ref[core]).astype(BF)

                qbuf[:, cols] = turned(total(0))
                kvbuf[j % 2, core, 0, :, cols] = turned(total(1))
                kvbuf[j % 2, core, 1, :, cols] = total(2)
            kv_copy(j).start()
            kv_copy(j).wait()
            q_pos = core * rows + lax.broadcasted_iota(jnp.int32, (rows, 2 * rows), 0)
            allowed = q_pos >= lax.broadcasted_iota(jnp.int32, (rows, 2 * rows), 1)
            for h in range(heads):
                cols = slice(h * HEAD_DIM, (h + 1) * HEAD_DIM)
                keys = kvbuf[j % 2, :, 0, :, cols].reshape(2 * rows, HEAD_DIM)
                vals = kvbuf[j % 2, :, 1, :, cols].reshape(2 * rows, HEAD_DIM)
                scores = lax.dot_general(qbuf[:, cols], keys, (((1,), (1,)), ((), ())), preferred_element_type=F32) * HEAD_DIM ** -0.5
                scores = jnp.where(allowed, scores, -1e30)
                weight = jnp.exp(scores - jnp.max(scores, axis=1, keepdims=True))
                prob = (weight / jnp.sum(weight, axis=1, keepdims=True)).astype(BF)
                abuf[j % 3, core, ypos, :, cols] = jnp.dot(prob, vals, preferred_element_type=F32).astype(BF)
            out_y_copy(j).start()

        @pl.when(i >= 2)
        def _():
            j = i - 2
            out_y_copy(j).wait()
            out_core_copy(j).start()

            @pl.when(j >= 3)
            def _():
                scatter_copy(j - 2, 0).wait_send()
                scatter_copy(j - 2, 1).wait_send()

            out_core_copy(j).wait()

            def out_half(half, carry):
                def out(t, carry):
                    cols = pl.ds(pl.multiple_of(t * 256, 256), 256)
                    part = jnp.dot(abuf[j % 3, half, 0], w_out[0:half_cols, cols], preferred_element_type=F32)
                    part += jnp.dot(abuf[j % 3, half, 1], w_out[half_cols:, cols], preferred_element_type=F32)

                    @pl.when(j == 0)
                    def _():
                        own[half, :, cols] = part

                    @pl.when(j > 0)
                    def _():
                        zsend[j % 2, half, :, cols] = part.astype(BF)
                    return carry

                lax.fori_loop(0, width // 256, out, 0)

                @pl.when(j > 0)
                def _():
                    scatter_copy(j, half).start()
                return carry

            lax.fori_loop(0, 2, out_half, 0)
        return carry

    lax.fori_loop(0, steps + 2, step, 0)

    @pl.when(z < 3)
    def _():
        to_right.wait_send()

    @pl.when(z > 0)
    def _():
        to_left.wait_send()

    @pl.when((z > 0) & (z < 3))
    def _():
        on_right.wait_send()
        on_left.wait_send()
        to_end.wait_send()

    for half in range(2):
        for j in (steps - 2, steps - 1):
            scatter_copy(j, half).wait_send()
        for by in (1, 2, 3):
            remote(zsend.at[0, half], zrecv.at[by - 1, half], zr_send.at[0, half], zr_recv.at[by - 1, half], {"ty": flip(z, by)}).wait_recv()

        def finish(t, carry):
            part = pl.ds(pl.multiple_of(t * 32, 32), 32)
            total = own[half, part]
            for by in range(3):
                total += zrecv[by, half, part].astype(F32)
            out_ref[half, part] = (x_ref[half, part].astype(F32) + total.astype(BF).astype(F32)).astype(BF)
            return carry

        lax.fori_loop(0, rows // 32, finish, 0)


def attention(x, w_q, w_k, w_v, w_o):
    seq_len, width = x.shape
    rows, half_cols = seq_len // 2, width // 2
    cos_t, sin_t = rot_tables(seq_len)
    dma, vmem = pltpu.SemaphoreType.DMA, pltpu.VMEM
    in_vmem, anywhere = pl.BlockSpec(memory_space=pltpu.VMEM), pl.BlockSpec(memory_space=pl.ANY)
    out = pl.pallas_call(
        attn_kernel,
        name="attention",
        out_shape=jax.ShapeDtypeStruct((2, rows, width), BF),
        in_specs=[in_vmem] * 3 + [anywhere] * 4,
        out_specs=in_vmem,
        scratch_shapes=[
            vmem((4, 2, rows, width), BF),
            vmem((3, width, width), BF),
            vmem((width, width), BF),
            vmem((2, 2, 3, rows, half_cols), BF),
            vmem((2, 2, 3, rows, half_cols), BF),
            vmem((2, 2, 3, rows, half_cols), BF),
            vmem((3, 3, rows, half_cols), BF),
            vmem((rows, half_cols), BF),
            vmem((2, 2, 2, rows, half_cols), BF),
            vmem((3, 2, 2, rows, half_cols), BF),
            vmem((2, 2, rows, width), BF),
            vmem((3, 2, rows, width), BF),
            vmem((2, rows, width), F32),
            vmem((4, 8, seq_len), F32), dma((2,)), dma((2,)),
            dma((4,)), dma((5,)), dma((4,)),
            dma((2,)), dma((2,)), dma((3,)), dma((3,)), dma((2,)), dma((2,)),
            dma((3,)), dma((3,)), dma((3,)), dma((3,)),
            dma((2, 2)), dma((3, 2)),
        ],
        compiler_params=pltpu.CompilerParams(collective_id=1, has_side_effects=True, vmem_limit_bytes=VMEM_LIMIT),
    )(x.reshape(2, rows, width), jnp.asarray(cos_t).reshape(2, rows, HEAD_DIM), jnp.asarray(sin_t).reshape(2, rows, HEAD_DIM), w_q, w_k, w_v, w_o)
    return out.reshape(seq_len, width)


def mlp_kernel(h_ref, wg_hbm, wu_hbm, wd_hbm, out_ref, xall, w_in, w_out, pbuf, r1, sbuf, r2, abuf, zsend, zrecv, own,
               stats, s_send, s_recv, w_sem, az_send, az_recv, p_send, p_recv, ry_send, ry_recv, ay_send, ay_recv, ac_send, ac_recv, zr_send, zr_recv):
    z, me = lax.axis_index("ty"), lax.axis_index("tx")
    core, ypos = me % 2, me // 2
    core_peer, y_peer = {"tx": flip(me, 1)}, {"tx": flip(me, 2)}
    halves, rows, width = h_ref.shape
    ff = wg_hbm.shape[1]
    tiles = ff // TILE
    all_tiles = 2 * tiles
    quarter = rows // 4
    steps = 4 * halves

    def slot(i):
        return ((i + 1) // 2) % 4, (i + 1) % 2

    def gather_copy(by, half):
        return remote(xall.at[0, half], xall.at[by, half], az_send.at[by, half], az_recv.at[by, half], {"ty": flip(z, by)})

    def core_copy(i, part):
        group = pl.ds(part * tiles, tiles)
        return remote(pbuf.at[1 - core, group], r1.at[i % 2, group], p_send.at[i % 2, part], p_recv.at[i % 2, part], core_peer)

    def y_copy(i, part):
        group = pl.ds(part * tiles, tiles)
        return remote(sbuf.at[i % 2, 1 - ypos, group], r2.at[i % 3, group], ry_send.at[i % 3, part], ry_recv.at[i % 3, part], y_peer)

    def act_y_copy(i):
        piece = abuf.at[i % 3, core, ypos]
        return remote(piece, piece, ay_send.at[i % 3], ay_recv.at[i % 3], y_peer)

    def act_core_copy(i):
        piece = abuf.at[i % 3, core]
        return remote(piece, piece, ac_send.at[i % 3], ac_recv.at[i % 3], core_peer)

    def scatter_copy(i):
        by, half = slot(i)
        return remote(zsend.at[i % 2], zrecv.at[by - 1, half], zr_send.at[i % 2], zr_recv.at[by - 1, half], {"ty": flip(z, by)})

    loads = [
        pltpu.make_async_copy(wg_hbm, w_in.at[:, pl.ds(0, ff)], w_sem.at[0]),
        pltpu.make_async_copy(wu_hbm, w_in.at[:, pl.ds(ff, ff)], w_sem.at[1]),
        pltpu.make_async_copy(wd_hbm, w_out, w_sem.at[2]),
    ]
    for load in loads:
        load.start()
    greet(z, me)
    norm_rows(h_ref, xall.at[0], stats, s_send, s_recv, core_peer, y_peer)
    for by in (1, 2, 3):
        for half in range(halves):
            gather_copy(by, half).start()
    loads[0].wait()
    loads[1].wait()

    def step(i, carry):
        @pl.when(i < steps)
        def _():
            by, half = slot(i)

            @pl.when((i > 0) & (i < steps - 1))
            def _():
                gather_copy(by, half).wait_recv()

            def product(t, carry):
                cols = pl.ds(pl.multiple_of(t * 2 * TILE, 2 * TILE), 2 * TILE)
                part = jnp.dot(xall[by, half], w_in[:, cols], preferred_element_type=F32).astype(BF)
                pbuf[:, 2 * t] = part[:, :TILE].reshape(2, 2, quarter, TILE)
                pbuf[:, 2 * t + 1] = part[:, TILE:].reshape(2, 2, quarter, TILE)
                return carry

            first = (tiles + 1) // 2
            lax.fori_loop(0, first, product, 0)
            core_copy(i, 0).start()
            lax.fori_loop(first, tiles, product, 0)
            core_copy(i, 1).start()
            for part in range(2):
                core_copy(i, part).wait_recv()

                def add(t, carry):
                    total = pbuf[core, t].astype(F32) + r1[i % 2, t].astype(F32)
                    total = total.astype(BF)
                    sbuf[i % 2, 0, t] = total[0]
                    sbuf[i % 2, 1, t] = total[1]
                    return carry

                lax.fori_loop(part * tiles, (part + 1) * tiles, add, 0)
                y_copy(i, part).start()
            for part in range(2):
                core_copy(i, part).wait_send()

        @pl.when((i >= 1) & (i <= steps))
        def _():
            j = i - 1
            for part in range(2):
                y_copy(j, part).wait()

            def gate(t, carry):
                g = (sbuf[j % 2, ypos, t].astype(F32) + r2[j % 3, t].astype(F32)).astype(BF).astype(F32)
                u = (sbuf[j % 2, ypos, tiles + t].astype(F32) + r2[j % 3, tiles + t].astype(F32)).astype(BF).astype(F32)
                cols = pl.ds(pl.multiple_of(t * TILE, TILE), TILE)
                abuf[j % 3, core, ypos, :, cols] = (g * jax.nn.sigmoid(g) * u).astype(BF)
                return carry

            lax.fori_loop(0, tiles, gate, 0)
            act_y_copy(j).start()

        @pl.when(i >= 2)
        def _():
            j = i - 2
            by, half = slot(j)
            act_y_copy(j).wait()
            act_core_copy(j).start()

            @pl.when(j == 0)
            def _():
                loads[2].wait()

            @pl.when((j >= 3) & (j < steps - 1))
            def _():
                scatter_copy(j - 2).wait_send()

            act_core_copy(j).wait()

            def down(t, carry):
                cols = pl.ds(pl.multiple_of(t * 256, 256), 256)
                part = jnp.dot(abuf[j % 3].reshape(rows, ff), w_out[:, cols], preferred_element_type=F32)

                @pl.when(by == 0)
                def _():
                    own[half, :, cols] = part

                @pl.when(by > 0)
                def _():
                    zsend[j % 2, :, cols] = part.astype(BF)
                return carry

            lax.fori_loop(0, width // 256, down, 0)

            @pl.when(by > 0)
            def _():
                scatter_copy(j).start()
        return carry

    lax.fori_loop(0, steps + 2, step, 0)

    for j in (steps - 3, steps - 2):
        scatter_copy(j).wait_send()
    for half in range(halves):
        for by in (1, 2, 3):
            gather_copy(by, half).wait_send()
            remote(zsend.at[0], zrecv.at[by - 1, half], zr_send.at[0], zr_recv.at[by - 1, half], {"ty": flip(z, by)}).wait_recv()

        def finish(t, carry):
            part = pl.ds(pl.multiple_of(t * 32, 32), 32)
            total = own[half, part]
            for by in range(3):
                total += zrecv[by, half, part].astype(F32)
            out_ref[half, part] = (h_ref[half, part].astype(F32) + total.astype(BF).astype(F32)).astype(BF)
            return carry

        lax.fori_loop(0, rows // 32, finish, 0)


def mlp(h, w_gate, w_up, w_down):
    seq_len, width = h.shape
    ff = w_gate.shape[1]
    halves = 2
    rows = seq_len // halves
    quarter = rows // 4
    tiles = ff // TILE
    dma, vmem = pltpu.SemaphoreType.DMA, pltpu.VMEM
    in_vmem, anywhere = pl.BlockSpec(memory_space=pltpu.VMEM), pl.BlockSpec(memory_space=pl.ANY)
    out = pl.pallas_call(
        mlp_kernel,
        name="mlp",
        out_shape=jax.ShapeDtypeStruct((halves, rows, width), BF),
        in_specs=[in_vmem, anywhere, anywhere, anywhere],
        out_specs=in_vmem,
        scratch_shapes=[
            vmem((4, halves, rows, width), BF),
            vmem((width, 2 * ff), BF),
            vmem((ff, width), BF),
            vmem((2, 2 * tiles, 2, quarter, TILE), BF),
            vmem((2, 2 * tiles, 2, quarter, TILE), BF),
            vmem((2, 2, 2 * tiles, quarter, TILE), BF),
            vmem((3, 2 * tiles, quarter, TILE), BF),
            vmem((3, 2, 2, quarter, ff), BF),
            vmem((2, rows, width), BF),
            vmem((3, halves, rows, width), BF),
            vmem((halves, rows, width), F32),
            vmem((4, 8, seq_len), F32), dma((2,)), dma((2,)),
            dma((3,)), dma((4, halves)), dma((4, halves)),
            dma((2, 2)), dma((2, 2)), dma((3, 2)), dma((3, 2)),
            dma((3,)), dma((3,)), dma((3,)), dma((3,)),
            dma((2,)), dma((3, halves)),
        ],
        compiler_params=pltpu.CompilerParams(collective_id=0, has_side_effects=True, vmem_limit_bytes=VMEM_LIMIT),
    )(h.reshape(halves, rows, width), w_gate, w_up, w_down)
    return out.reshape(seq_len, width)


def solution(mesh):
    act_spec = P(("dp", "ty"), None, "tx")
    col_spec = P("tx", "ty")
    row_spec = P("ty", "tx")

    def layer_fn(x_blk, w_q, w_k, w_v, w_o, w_gate, w_up, w_down):
        h = attention(x_blk[0], w_q, w_k, w_v, w_o)
        return mlp(h, w_gate, w_up, w_down)[None]

    return jax.shard_map(layer_fn, mesh=mesh, in_specs=(act_spec, col_spec, col_spec, col_spec, row_spec, col_spec, col_spec, row_spec), out_specs=act_spec, check_vma=False)
```

```python
import jax
import jax.numpy as jnp
import numpy as np
from jax import lax
from jax.experimental import pallas as pl
from jax.experimental.pallas import tpu as pltpu
from jax.sharding import PartitionSpec as P

HEAD_DIM = 128
EPS = 1e-5
THETA = 10000.0
BF = jnp.bfloat16
F32 = jnp.float32


def rot_tables(seq_len):
    half_dim = HEAD_DIM // 2
    inv_freq = np.float32(THETA) ** (-2.0 * np.arange(half_dim, dtype=np.float32) / np.float32(HEAD_DIM))
    angles = np.arange(seq_len, dtype=np.float32)[:, None] * inv_freq.astype(np.float32)[None, :]
    cos_t, sin_t = np.cos(angles), np.sin(angles)
    return np.concatenate([cos_t, cos_t], -1), np.concatenate([-sin_t, sin_t], -1)


MESH = pl.DeviceIdType.MESH
TILE = 384
VMEM_LIMIT = 67043328


def flip(index, by):
    low, high = index % 2, index // 2
    by_low, by_high = by % 2, by // 2
    return low + by_low - 2 * low * by_low + 2 * (high + by_high - 2 * high * by_high)


def greet(z, me):
    barrier = pltpu.get_barrier_semaphore()
    for by in (1, 2, 3):
        pl.semaphore_signal(barrier, inc=1, device_id={"ty": flip(z, by)}, device_id_type=MESH)
    pl.semaphore_signal(barrier, inc=1, device_id={"tx": flip(me, 1)}, device_id_type=MESH)
    pl.semaphore_signal(barrier, inc=1, device_id={"tx": flip(me, 2)}, device_id_type=MESH)
    pl.semaphore_wait(barrier, 5)


def norm_rows(src, dst, stats, send_sem, recv_sem, core_peer, y_peer, ready):
    halves, rows, width = src.shape
    total_rows = halves * rows
    full_width = 4 * width
    lane = lax.broadcasted_iota(jnp.int32, (rows, 128), 1)
    for half in range(halves):
        vals = src[half].astype(F32)
        both = jnp.where(lane == 0, jnp.sum(vals, axis=1, keepdims=True), jnp.sum(vals * vals, axis=1, keepdims=True))
        stats[0, :, half * rows:(half + 1) * rows] = both.T[:8]
    swap = remote(stats.at[0], stats.at[1], send_sem.at[0], recv_sem.at[0], core_peer)
    swap.start()
    swap.wait()
    stats[2] = stats[0] + stats[1]
    swap = remote(stats.at[2], stats.at[3], send_sem.at[1], recv_sem.at[1], y_peer)
    swap.start()
    swap.wait()
    sums = stats[2] + stats[3]
    sums = jnp.concatenate([sums, jnp.zeros((120, total_rows), F32)], 0).T
    mean_val = sums[:, 0:1] / full_width
    var_val = sums[:, 1:2] / full_width - mean_val * mean_val
    scale = lax.rsqrt(var_val + EPS)
    for half in range(halves):
        part = slice(half * rows, (half + 1) * rows)
        dst[half] = ((src[half].astype(F32) - mean_val[part]) * scale[part]).astype(BF)
        ready(half)


def remote(src, dst, send_sem, recv_sem, device_id):
    return pltpu.make_async_remote_copy(src_ref=src, dst_ref=dst, send_sem=send_sem, recv_sem=recv_sem, device_id=device_id, device_id_type=MESH)


def attn_kernel(x_ref, cos_ref, sin_ref, wq_hbm, wk_hbm, wv_hbm, wo_hbm, out_ref, xall, w_in, w_out, pbuf, r1, sbuf, r2, qbuf, kvbuf, abuf, zsend, zrecv, own,
                stats, s_send, s_recv, w_sem, az_send, az_recv, p_send, p_recv, ry_send, ry_recv, kv_send, kv_recv, ay_send, ay_recv, ac_send, ac_recv, zr_send, zr_recv):
    z, me = lax.axis_index("ty"), lax.axis_index("tx")
    core, ypos = me % 2, me // 2
    core_peer, y_peer = {"tx": flip(me, 1)}, {"tx": flip(me, 2)}
    halves, rows, width = x_ref.shape
    piece_rows = rows // 2
    half_cols = width // 2
    heads = half_cols // HEAD_DIM
    steps = 4 * halves
    inner = flip(z % 2, z // 2)

    def slot(i):
        turn = ((i + 1) // 2) % 4
        edge = 1 - (i * (steps - 1 - i) + 11) // 12
        return inner * ((4 - turn) % 4) + (1 - inner) * turn, (i + 1 + edge) % 2

    right_slot, left_slot = 1 + 2 * (z % 2), 3 - 2 * (z % 2)

    def to_right(half):
        return remote(xall.at[0, half], xall.at[right_slot, half], az_send.at[0, half], az_recv.at[right_slot, half], {"ty": (z + 1) % 4})

    def to_left(half):
        return remote(xall.at[0, half], xall.at[left_slot, half], az_send.at[1, half], az_recv.at[left_slot, half], {"ty": (z + 3) % 4})

    def on_right(half):
        return remote(xall.at[left_slot, half], xall.at[2, half], az_send.at[2, half], az_recv.at[2, half], {"ty": (z + 1) % 4})

    def on_left(half):
        return remote(xall.at[right_slot, half], xall.at[2, half], az_send.at[3, half], az_recv.at[2, half], {"ty": (z + 3) % 4})

    def to_end(half):
        return remote(xall.at[2, half], xall.at[3, half], az_send.at[4, half], az_recv.at[3, half], {"ty": (3 * z + 1) % 4})

    def arrived(by, half):
        remote(xall.at[by, half], xall.at[by, half], az_send.at[0, half], az_recv.at[by, half], {"ty": flip(z, 1)}).wait_recv()

    def core_copy(i):
        return remote(pbuf.at[1 - core], r1.at[i % 2], p_send.at[i % 2], p_recv.at[i % 2], core_peer)

    def y_copy(i):
        return remote(sbuf.at[i % 2, 1 - ypos], r2.at[i % 3], ry_send.at[i % 3], ry_recv.at[i % 3], y_peer)

    def kv_copy(i):
        by, half = slot(i)
        piece = kvbuf.at[by, half, core]
        return remote(piece, piece, kv_send.at[by, half], kv_recv.at[by, half], core_peer)

    def out_y_copy(i):
        piece = abuf.at[i % 3, core, ypos]
        return remote(piece, piece, ay_send.at[i % 3], ay_recv.at[i % 3], y_peer)

    def out_core_copy(i):
        piece = abuf.at[i % 3, core]
        return remote(piece, piece, ac_send.at[i % 3], ac_recv.at[i % 3], core_peer)

    def scatter_copy(i):
        by, half = slot(i)
        return remote(zsend.at[i % 2], zrecv.at[by - 1, half], zr_send.at[i % 2], zr_recv.at[by - 1, half], {"ty": flip(z, by)})

    loads = [pltpu.make_async_copy(w, w_in.at[n], w_sem.at[n]) for n, w in enumerate((wq_hbm, wk_hbm, wv_hbm))]
    loads.append(pltpu.make_async_copy(wo_hbm, w_out, w_sem.at[3]))
    for load in loads:
        load.start()
    greet(z, me)

    def send_own(half):
        @pl.when(z < 3)
        def _():
            to_right(half).start()

        @pl.when(z > 0)
        def _():
            to_left(half).start()

    norm_rows(x_ref, xall.at[0], stats, s_send, s_recv, core_peer, y_peer, send_own)
    for load in loads:
        load.wait()

    def step(i, carry):
        @pl.when(i < steps)
        def _():
            by, half = slot(i)
            first = (i >= 1) & (i <= 2)

            @pl.when(first & (z > 0))
            def _():
                arrived(left_slot, half)

            @pl.when(first & (z > 0) & (z < 3))
            def _():
                on_right(half).start()

            @pl.when(first & (z < 3))
            def _():
                arrived(right_slot, half)

            @pl.when(first & (z > 0) & (z < 3))
            def _():
                on_left(half).start()

            second = (i >= 3) & (i <= 4)

            @pl.when(second)
            def _():
                arrived(2, half)

            @pl.when(second & (z > 0) & (z < 3))
            def _():
                to_end(half).start()

            @pl.when((i >= 5) & (i <= 6) & (z != 1) & (z != 2))
            def _():
                arrived(3, half)

            def product(t, carry):
                part = jnp.dot(xall[by, half], w_in[t], preferred_element_type=F32).astype(BF)
                for side in range(2):
                    block = slice(side * piece_rows, (side + 1) * piece_rows)
                    pbuf[side, 0, t] = part[block, :half_cols]
                    pbuf[side, 1, t] = part[block, half_cols:]
                return carry

            lax.fori_loop(0, 3, product, 0)
            core_copy(i).start()
            core_copy(i).wait()

            def add(t, carry):
                for side in range(2):
                    sbuf[i % 2, side, t] = (pbuf[core, side, t].astype(F32) + r1[i % 2, side, t].astype(F32)).astype(BF)
                return carry

            lax.fori_loop(0, 3, add, 0)
            y_copy(i).start()

        @pl.when((i >= 1) & (i <= steps))
        def _():
            j = i - 1
            by, half = slot(j)
            y_copy(j).wait()
            for h in range(heads):
                cols = slice(h * HEAD_DIM, (h + 1) * HEAD_DIM)

                def total(n):
                    return (sbuf[j % 2, ypos, n, :, cols].astype(F32) + r2[j % 3, n, :, cols].astype(F32)).astype(BF)

                def turned(vals):
                    vals = vals.astype(F32)
                    return (vals * cos_ref[half, core] + pltpu.roll(vals, HEAD_DIM // 2, 1) * sin_ref[half, core]).astype(BF)

                qbuf[:, cols] = turned(total(0))
                kvbuf[by, half, core, 0, :, cols] = turned(total(1))
                kvbuf[by, half, core, 1, :, cols] = total(2)
            kv_copy(j).start()
            kv_copy(j).wait()

            def attend(n_halves):
                n_keys = n_halves * rows
                q_pos = (n_halves - 1) * rows + core * piece_rows + lax.broadcasted_iota(jnp.int32, (piece_rows, n_keys), 0)
                allowed = q_pos >= lax.broadcasted_iota(jnp.int32, (piece_rows, n_keys), 1)
                for h in range(heads):
                    cols = slice(h * HEAD_DIM, (h + 1) * HEAD_DIM)
                    keys = kvbuf[by, :n_halves, :, 0, :, cols].reshape(n_keys, HEAD_DIM)
                    vals = kvbuf[by, :n_halves, :, 1, :, cols].reshape(n_keys, HEAD_DIM)
                    scores = lax.dot_general(qbuf[:, cols], keys, (((1,), (1,)), ((), ())), preferred_element_type=F32) * HEAD_DIM ** -0.5
                    scores = jnp.where(allowed, scores, -1e30)
                    weight = jnp.exp(scores - jnp.max(scores, axis=1, keepdims=True))
                    prob = (weight / jnp.sum(weight, axis=1, keepdims=True)).astype(BF)
                    abuf[j % 3, core, ypos, :, cols] = jnp.dot(prob, vals, preferred_element_type=F32).astype(BF)

            @pl.when(half == 0)
            def _():
                attend(1)

            @pl.when(half == 1)
            def _():
                attend(2)

            out_y_copy(j).start()

        @pl.when(i >= 2)
        def _():
            j = i - 2
            by, half = slot(j)
            out_y_copy(j).wait()
            out_core_copy(j).start()

            @pl.when((j >= 3) & (j < steps - 1))
            def _():
                scatter_copy(j - 2).wait_send()

            out_core_copy(j).wait()

            def out(t, carry):
                cols = pl.ds(pl.multiple_of(t * 256, 256), 256)
                part = jnp.dot(abuf[j % 3, :, 0].reshape(rows, half_cols), w_out[0:half_cols, cols], preferred_element_type=F32)
                part += jnp.dot(abuf[j % 3, :, 1].reshape(rows, half_cols), w_out[half_cols:, cols], preferred_element_type=F32)

                @pl.when(by == 0)
                def _():
                    own[half, :, cols] = part

                @pl.when(by > 0)
                def _():
                    zsend[j % 2, :, cols] = part.astype(BF)
                return carry

            lax.fori_loop(0, width // 256, out, 0)

            @pl.when(by > 0)
            def _():
                scatter_copy(j).start()
        return carry

    lax.fori_loop(0, steps + 2, step, 0)

    for half in range(halves):
        @pl.when(z < 3)
        def _():
            to_right(half).wait_send()

        @pl.when(z > 0)
        def _():
            to_left(half).wait_send()

        @pl.when((z > 0) & (z < 3))
        def _():
            on_right(half).wait_send()
            on_left(half).wait_send()
            to_end(half).wait_send()

    for j in (steps - 3, steps - 2):
        scatter_copy(j).wait_send()
    for half in range(halves):
        for by in (1, 2, 3):
            remote(zsend.at[0], zrecv.at[by - 1, half], zr_send.at[0], zr_recv.at[by - 1, half], {"ty": flip(z, by)}).wait_recv()

        def finish(t, carry):
            part = pl.ds(pl.multiple_of(t * 32, 32), 32)
            total = own[half, part]
            for by in range(3):
                total += zrecv[by, half, part].astype(F32)
            out_ref[half, part] = (x_ref[half, part].astype(F32) + total.astype(BF).astype(F32)).astype(BF)
            return carry

        lax.fori_loop(0, rows // 32, finish, 0)


def attention(x, w_q, w_k, w_v, w_o):
    seq_len, width = x.shape
    rows, half_cols = seq_len // 2, width // 2
    piece_rows = rows // 2
    cos_t, sin_t = rot_tables(seq_len)
    dma, vmem = pltpu.SemaphoreType.DMA, pltpu.VMEM
    in_vmem, anywhere = pl.BlockSpec(memory_space=pltpu.VMEM), pl.BlockSpec(memory_space=pl.ANY)
    out = pl.pallas_call(
        attn_kernel,
        name="attention",
        out_shape=jax.ShapeDtypeStruct((2, rows, width), BF),
        in_specs=[in_vmem] * 3 + [anywhere] * 4,
        out_specs=in_vmem,
        scratch_shapes=[
            vmem((4, 2, rows, width), BF),
            vmem((3, width, width), BF),
            vmem((width, width), BF),
            vmem((2, 2, 3, piece_rows, half_cols), BF),
            vmem((2, 2, 3, piece_rows, half_cols), BF),
            vmem((2, 2, 3, piece_rows, half_cols), BF),
            vmem((3, 3, piece_rows, half_cols), BF),
            vmem((piece_rows, half_cols), BF),
            vmem((4, 2, 2, 2, piece_rows, half_cols), BF),
            vmem((3, 2, 2, piece_rows, half_cols), BF),
            vmem((2, rows, width), BF),
            vmem((3, 2, rows, width), BF),
            vmem((2, rows, width), F32),
            vmem((4, 8, seq_len), F32), dma((2,)), dma((2,)),
            dma((4,)), dma((5, 2)), dma((4, 2)),
            dma((2,)), dma((2,)), dma((3,)), dma((3,)), dma((4, 2)), dma((4, 2)),
            dma((3,)), dma((3,)), dma((3,)), dma((3,)),
            dma((2,)), dma((3, 2)),
        ],
        compiler_params=pltpu.CompilerParams(collective_id=1, has_side_effects=True, vmem_limit_bytes=VMEM_LIMIT),
    )(x.reshape(2, rows, width), jnp.asarray(cos_t).reshape(2, 2, piece_rows, HEAD_DIM), jnp.asarray(sin_t).reshape(2, 2, piece_rows, HEAD_DIM), w_q, w_k, w_v, w_o)
    return out.reshape(seq_len, width)


def mlp_kernel(h_ref, wg_hbm, wu_hbm, wd_hbm, out_ref, xall, w_in, w_out, pbuf, r1, sbuf, r2, abuf, zsend, zrecv, own,
               stats, s_send, s_recv, w_sem, az_send, az_recv, p_send, p_recv, ry_send, ry_recv, ay_send, ay_recv, ac_send, ac_recv, zr_send, zr_recv):
    z, me = lax.axis_index("ty"), lax.axis_index("tx")
    core, ypos = me % 2, me // 2
    core_peer, y_peer = {"tx": flip(me, 1)}, {"tx": flip(me, 2)}
    halves, rows, width = h_ref.shape
    ff = wg_hbm.shape[1]
    tiles = ff // TILE
    all_tiles = 2 * tiles
    quarter = rows // 4
    steps = 4 * halves
    pairs = ((0, (tiles + 1) // 2), ((tiles + 1) // 2, tiles))

    def slot(i):
        return ((i + 1) // 2) % 4, (i + 1) % 2

    right_slot, left_slot = 1 + 2 * (z % 2), 3 - 2 * (z % 2)

    def to_right(half):
        return remote(xall.at[0, half], xall.at[right_slot, half], az_send.at[0, half], az_recv.at[right_slot, half], {"ty": (z + 1) % 4})

    def to_left(half):
        return remote(xall.at[0, half], xall.at[left_slot, half], az_send.at[1, half], az_recv.at[left_slot, half], {"ty": (z + 3) % 4})

    def on_right(half):
        return remote(xall.at[left_slot, half], xall.at[2, half], az_send.at[2, half], az_recv.at[2, half], {"ty": (z + 1) % 4})

    def on_left(half):
        return remote(xall.at[right_slot, half], xall.at[2, half], az_send.at[3, half], az_recv.at[2, half], {"ty": (z + 3) % 4})

    def to_end(half):
        return remote(xall.at[2, half], xall.at[3, half], az_send.at[4, half], az_recv.at[3, half], {"ty": (3 * z + 1) % 4})

    def arrived(by, half):
        remote(xall.at[by, half], xall.at[by, half], az_send.at[0, half], az_recv.at[by, half], {"ty": flip(z, 1)}).wait_recv()

    def core_copy(i, part):
        group = pl.ds(2 * pairs[part][0], 2 * (pairs[part][1] - pairs[part][0]))
        return remote(pbuf.at[1 - core, group], r1.at[i % 2, group], p_send.at[i % 2, part], p_recv.at[i % 2, part], core_peer)

    def y_copy(i, part):
        group = pl.ds(2 * pairs[part][0], 2 * (pairs[part][1] - pairs[part][0]))
        return remote(sbuf.at[i % 2, 1 - ypos, group], r2.at[i % 3, group], ry_send.at[i % 3, part], ry_recv.at[i % 3, part], y_peer)

    def act_y_copy(i, part):
        cols = pl.ds(pairs[part][0] * TILE, (pairs[part][1] - pairs[part][0]) * TILE)
        piece = abuf.at[i % 3, core, ypos, :, cols]
        return remote(piece, piece, ay_send.at[i % 3, part], ay_recv.at[i % 3, part], y_peer)

    def act_core_copy(i):
        piece = abuf.at[i % 3, core]
        return remote(piece, piece, ac_send.at[i % 3], ac_recv.at[i % 3], core_peer)

    def scatter_copy(i):
        by, half = slot(i)
        return remote(zsend.at[i % 2], zrecv.at[by - 1, half], zr_send.at[i % 2], zr_recv.at[by - 1, half], {"ty": flip(z, by)})

    loads = [
        pltpu.make_async_copy(wg_hbm, w_in.at[:, pl.ds(0, ff)], w_sem.at[0]),
        pltpu.make_async_copy(wu_hbm, w_in.at[:, pl.ds(ff, ff)], w_sem.at[1]),
        pltpu.make_async_copy(wd_hbm, w_out, w_sem.at[2]),
    ]
    for load in loads:
        load.start()
    greet(z, me)

    def send_own(half):
        @pl.when(z < 3)
        def _():
            to_right(half).start()

        @pl.when(z > 0)
        def _():
            to_left(half).start()

    norm_rows(h_ref, xall.at[0], stats, s_send, s_recv, core_peer, y_peer, send_own)
    loads[0].wait()
    loads[1].wait()

    def step(i, carry):
        @pl.when(i < steps)
        def _():
            by, half = slot(i)

            first = (i >= 1) & (i <= 2)

            @pl.when(first & (z > 0))
            def _():
                arrived(left_slot, half)

            @pl.when(first & (z > 0) & (z < 3))
            def _():
                on_right(half).start()

            @pl.when(first & (z < 3))
            def _():
                arrived(right_slot, half)

            @pl.when(first & (z > 0) & (z < 3))
            def _():
                on_left(half).start()

            second = (i >= 3) & (i <= 4)

            @pl.when(second)
            def _():
                arrived(2, half)

            @pl.when(second & (z > 0) & (z < 3))
            def _():
                to_end(half).start()

            @pl.when((i >= 5) & (i <= 6) & (z != 1) & (z != 2))
            def _():
                arrived(3, half)

            def product(t, carry):
                for side in range(2):
                    cols = pl.ds(pl.multiple_of(side * ff + t * TILE, TILE), TILE)
                    part = jnp.dot(xall[by, half], w_in[:, cols], preferred_element_type=F32).astype(BF)
                    pbuf[:, 2 * t + side] = part.reshape(2, 2, quarter, TILE)
                return carry

            for part in range(2):
                lax.fori_loop(*pairs[part], product, 0)
                core_copy(i, part).start()
            for part in range(2):
                core_copy(i, part).wait_recv()

                def add(t, carry):
                    total = pbuf[core, t].astype(F32) + r1[i % 2, t].astype(F32)
                    total = total.astype(BF)
                    sbuf[i % 2, 0, t] = total[0]
                    sbuf[i % 2, 1, t] = total[1]
                    return carry

                lax.fori_loop(2 * pairs[part][0], 2 * pairs[part][1], add, 0)
                y_copy(i, part).start()
            for part in range(2):
                core_copy(i, part).wait_send()

        @pl.when((i >= 1) & (i <= steps))
        def _():
            j = i - 1

            def gate(t, carry):
                g = (sbuf[j % 2, ypos, 2 * t].astype(F32) + r2[j % 3, 2 * t].astype(F32)).astype(BF).astype(F32)
                u = (sbuf[j % 2, ypos, 2 * t + 1].astype(F32) + r2[j % 3, 2 * t + 1].astype(F32)).astype(BF).astype(F32)
                cols = pl.ds(pl.multiple_of(t * TILE, TILE), TILE)
                abuf[j % 3, core, ypos, :, cols] = (g * jax.nn.sigmoid(g) * u).astype(BF)
                return carry

            for part in range(2):
                y_copy(j, part).wait()
                lax.fori_loop(*pairs[part], gate, 0)
                act_y_copy(j, part).start()

        @pl.when(i >= 2)
        def _():
            j = i - 2
            by, half = slot(j)
            act_y_copy(j, 0).wait()
            act_y_copy(j, 1).wait()
            act_core_copy(j).start()

            @pl.when(j == 0)
            def _():
                loads[2].wait()

            @pl.when((j >= 3) & (j < steps - 1))
            def _():
                scatter_copy(j - 2).wait_send()

            act_core_copy(j).wait()

            def down(t, carry):
                cols = pl.ds(pl.multiple_of(t * 256, 256), 256)
                part = jnp.dot(abuf[j % 3].reshape(rows, ff), w_out[:, cols], preferred_element_type=F32)

                @pl.when(by == 0)
                def _():
                    own[half, :, cols] = part

                @pl.when(by > 0)
                def _():
                    zsend[j % 2, :, cols] = part.astype(BF)
                return carry

            lax.fori_loop(0, width // 256, down, 0)

            @pl.when(by > 0)
            def _():
                scatter_copy(j).start()
        return carry

    lax.fori_loop(0, steps + 2, step, 0)

    for half in range(halves):
        @pl.when(z < 3)
        def _():
            to_right(half).wait_send()

        @pl.when(z > 0)
        def _():
            to_left(half).wait_send()

        @pl.when((z > 0) & (z < 3))
        def _():
            on_right(half).wait_send()
            on_left(half).wait_send()
            to_end(half).wait_send()

    for j in (steps - 3, steps - 2):
        scatter_copy(j).wait_send()
    for half in range(halves):
        for by in (1, 2, 3):
            remote(zsend.at[0], zrecv.at[by - 1, half], zr_send.at[0], zr_recv.at[by - 1, half], {"ty": flip(z, by)}).wait_recv()

        def finish(t, carry):
            part = pl.ds(pl.multiple_of(t * 32, 32), 32)
            total = own[half, part]
            for by in range(3):
                total += zrecv[by, half, part].astype(F32)
            out_ref[half, part] = (h_ref[half, part].astype(F32) + total.astype(BF).astype(F32)).astype(BF)
            return carry

        lax.fori_loop(0, rows // 32, finish, 0)


def mlp(h, w_gate, w_up, w_down):
    seq_len, width = h.shape
    ff = w_gate.shape[1]
    halves = 2
    rows = seq_len // halves
    quarter = rows // 4
    tiles = ff // TILE
    dma, vmem = pltpu.SemaphoreType.DMA, pltpu.VMEM
    in_vmem, anywhere = pl.BlockSpec(memory_space=pltpu.VMEM), pl.BlockSpec(memory_space=pl.ANY)
    out = pl.pallas_call(
        mlp_kernel,
        name="mlp",
        out_shape=jax.ShapeDtypeStruct((halves, rows, width), BF),
        in_specs=[in_vmem, anywhere, anywhere, anywhere],
        out_specs=in_vmem,
        scratch_shapes=[
            vmem((4, halves, rows, width), BF),
            vmem((width, 2 * ff), BF),
            vmem((ff, width), BF),
            vmem((2, 2 * tiles, 2, quarter, TILE), BF),
            vmem((2, 2 * tiles, 2, quarter, TILE), BF),
            vmem((2, 2, 2 * tiles, quarter, TILE), BF),
            vmem((3, 2 * tiles, quarter, TILE), BF),
            vmem((3, 2, 2, quarter, ff), BF),
            vmem((2, rows, width), BF),
            vmem((3, halves, rows, width), BF),
            vmem((halves, rows, width), F32),
            vmem((4, 8, seq_len), F32), dma((2,)), dma((2,)),
            dma((3,)), dma((5, halves)), dma((4, halves)),
            dma((2, 2)), dma((2, 2)), dma((3, 2)), dma((3, 2)),
            dma((3, 2)), dma((3, 2)), dma((3,)), dma((3,)),
            dma((2,)), dma((3, halves)),
        ],
        compiler_params=pltpu.CompilerParams(collective_id=0, has_side_effects=True, vmem_limit_bytes=VMEM_LIMIT),
    )(h.reshape(halves, rows, width), w_gate, w_up, w_down)
    return out.reshape(seq_len, width)


def solution(mesh):
    act_spec = P(("dp", "ty"), None, "tx")
    col_spec = P("tx", "ty")
    row_spec = P("ty", "tx")

    def layer_fn(x_blk, w_q, w_k, w_v, w_o, w_gate, w_up, w_down):
        h = attention(x_blk[0], w_q, w_k, w_v, w_o)
        return mlp(h, w_gate, w_up, w_down)[None]

    return jax.shard_map(layer_fn, mesh=mesh, in_specs=(act_spec, col_spec, col_spec, col_spec, row_spec, col_spec, col_spec, row_spec), out_specs=act_spec, check_vma=False)
```

```python
import jax
import jax.numpy as jnp
import numpy as np
from jax import lax
from jax.experimental import pallas as pl
from jax.experimental.pallas import tpu as pltpu
from jax.sharding import PartitionSpec as P

HEAD_DIM = 128
EPS = 1e-5
THETA = 10000.0
BF = jnp.bfloat16
F32 = jnp.float32


def rot_tables(seq_len):
    half_dim = HEAD_DIM // 2
    inv_freq = np.float32(THETA) ** (-2.0 * np.arange(half_dim, dtype=np.float32) / np.float32(HEAD_DIM))
    angles = np.arange(seq_len, dtype=np.float32)[:, None] * inv_freq.astype(np.float32)[None, :]
    cos_t, sin_t = np.cos(angles), np.sin(angles)
    return np.concatenate([cos_t, cos_t], -1), np.concatenate([-sin_t, sin_t], -1)


MESH = pl.DeviceIdType.MESH
TILE = 384
VMEM_LIMIT = 67043328


def flip(index, by):
    low, high = index % 2, index // 2
    by_low, by_high = by % 2, by // 2
    return low + by_low - 2 * low * by_low + 2 * (high + by_high - 2 * high * by_high)


def greet(z, me):
    barrier = pltpu.get_barrier_semaphore()
    for by in (1, 2, 3):
        pl.semaphore_signal(barrier, inc=1, device_id={"ty": flip(z, by)}, device_id_type=MESH)
    pl.semaphore_signal(barrier, inc=1, device_id={"tx": flip(me, 1)}, device_id_type=MESH)
    pl.semaphore_signal(barrier, inc=1, device_id={"tx": flip(me, 2)}, device_id_type=MESH)
    pl.semaphore_wait(barrier, 5)


def norm_rows(src, dst, stats, send_sem, recv_sem, core_peer, y_peer, ready):
    halves, rows, width = src.shape
    total_rows = halves * rows
    full_width = 4 * width
    lane = lax.broadcasted_iota(jnp.int32, (rows, 128), 1)
    for half in range(halves):
        vals = src[half].astype(F32)
        both = jnp.where(lane == 0, jnp.sum(vals, axis=1, keepdims=True), jnp.sum(vals * vals, axis=1, keepdims=True))
        stats[0, :, half * rows:(half + 1) * rows] = both.T[:8]
    swap = remote(stats.at[0], stats.at[1], send_sem.at[0], recv_sem.at[0], core_peer)
    swap.start()
    swap.wait()
    stats[2] = stats[0] + stats[1]
    swap = remote(stats.at[2], stats.at[3], send_sem.at[1], recv_sem.at[1], y_peer)
    swap.start()
    swap.wait()
    sums = stats[2] + stats[3]
    sums = jnp.concatenate([sums, jnp.zeros((120, total_rows), F32)], 0).T
    mean_val = sums[:, 0:1] / full_width
    var_val = sums[:, 1:2] / full_width - mean_val * mean_val
    scale = lax.rsqrt(var_val + EPS)
    for half in range(halves):
        part = slice(half * rows, (half + 1) * rows)
        dst[half] = ((src[half].astype(F32) - mean_val[part]) * scale[part]).astype(BF)
        ready(half)


def remote(src, dst, send_sem, recv_sem, device_id):
    return pltpu.make_async_remote_copy(src_ref=src, dst_ref=dst, send_sem=send_sem, recv_sem=recv_sem, device_id=device_id, device_id_type=MESH)


def attn_kernel(x_ref, cos_ref, sin_ref, wq_hbm, wk_hbm, wv_hbm, wo_hbm, out_ref, xall, w_in, w_out, pbuf, r1, sbuf, r2, qbuf, kvbuf, abuf, zsend, zrecv, cbuf, rbuf, own,
                stats, s_send, s_recv, w_sem, az_send, az_recv, p_send, p_recv, ry_send, ry_recv, kv_send, kv_recv, ay_send, ay_recv, ac_send, ac_recv, zr_send, zr_recv, rl_recv, cb_send):
    z, me = lax.axis_index("ty"), lax.axis_index("tx")
    core, ypos = me % 2, me // 2
    core_peer, y_peer = {"tx": flip(me, 1)}, {"tx": flip(me, 2)}
    halves, rows, width = x_ref.shape
    piece_rows = rows // 2
    half_cols = width // 2
    heads = half_cols // HEAD_DIM
    steps = 4 * halves
    inner = flip(z % 2, z // 2)

    def slot(i):
        turn = ((i + 1) // 2) % 4
        edge = 1 - (i * (steps - 1 - i) + 11) // 12
        return inner * ((4 - turn) % 4) + (1 - inner) * turn, (i + 1 + edge) % 2

    right_slot, left_slot = 1 + 2 * (z % 2), 3 - 2 * (z % 2)

    def to_right(half):
        return remote(xall.at[0, half], xall.at[right_slot, half], az_send.at[0, half], az_recv.at[right_slot, half], {"ty": (z + 1) % 4})

    def to_left(half):
        return remote(xall.at[0, half], xall.at[left_slot, half], az_send.at[1, half], az_recv.at[left_slot, half], {"ty": (z + 3) % 4})

    def on_right(half):
        return remote(xall.at[left_slot, half], xall.at[2, half], az_send.at[2, half], az_recv.at[2, half], {"ty": (z + 1) % 4})

    def on_left(half):
        return remote(xall.at[right_slot, half], xall.at[2, half], az_send.at[3, half], az_recv.at[2, half], {"ty": (z + 3) % 4})

    def to_end(half):
        return remote(xall.at[2, half], xall.at[3, half], az_send.at[4, half], az_recv.at[3, half], {"ty": (3 * z + 1) % 4})

    def arrived(by, half):
        remote(xall.at[by, half], xall.at[by, half], az_send.at[0, half], az_recv.at[by, half], {"ty": flip(z, 1)}).wait_recv()

    def core_copy(i):
        return remote(pbuf.at[1 - core], r1.at[i % 2], p_send.at[i % 2], p_recv.at[i % 2], core_peer)

    def y_copy(i):
        return remote(sbuf.at[i % 2, 1 - ypos], r2.at[i % 3], ry_send.at[i % 3], ry_recv.at[i % 3], y_peer)

    def kv_copy(i):
        by, half = slot(i)
        piece = kvbuf.at[by, half, core]
        return remote(piece, piece, kv_send.at[by, half], kv_recv.at[by, half], core_peer)

    def out_y_copy(i):
        piece = abuf.at[i % 3, core, ypos]
        return remote(piece, piece, ay_send.at[i % 3], ay_recv.at[i % 3], y_peer)

    def out_core_copy(i):
        piece = abuf.at[i % 3, core]
        return remote(piece, piece, ac_send.at[i % 3], ac_recv.at[i % 3], core_peer)

    def direct_copy(i):
        half = slot(i)[1]
        return remote(zsend.at[i % 2], zrecv.at[0, half], zr_send.at[i % 2], zr_recv.at[0, half], {"ty": flip(z, 1)})

    def relay_copy(i):
        half, far = slot(i)[1], ((i + 1) // 2) % 2
        return remote(zsend.at[i % 2], rbuf.at[far, half], zr_send.at[i % 2], rl_recv.at[far, half], {"ty": flip(z, 1)})

    def cross_copy(far, half):
        return remote(cbuf.at[far, half], zrecv.at[1, half], cb_send.at[far, half], zr_recv.at[1, half], {"ty": flip(z, 3 - far)})

    def combine(far, half):
        remote(cbuf.at[far, half], rbuf.at[far, half], cb_send.at[far, half], rl_recv.at[far, half], {"ty": flip(z, 1)}).wait_recv()

        def add(t, carry):
            part = pl.ds(pl.multiple_of(t * 32, 32), 32)
            cbuf[far, half, part] = (cbuf[far, half, part].astype(F32) + rbuf[far, half, part].astype(F32)).astype(BF)
            return carry

        lax.fori_loop(0, rows // 32, add, 0)
        cross_copy(far, half).start()

    loads = [pltpu.make_async_copy(w, w_in.at[n], w_sem.at[n]) for n, w in enumerate((wq_hbm, wk_hbm, wv_hbm))]
    loads.append(pltpu.make_async_copy(wo_hbm, w_out, w_sem.at[3]))
    for load in loads:
        load.start()
    greet(z, me)

    def send_own(half):
        @pl.when(z < 3)
        def _():
            to_right(half).start()

        @pl.when(z > 0)
        def _():
            to_left(half).start()

    norm_rows(x_ref, xall.at[0], stats, s_send, s_recv, core_peer, y_peer, send_own)
    for load in loads:
        load.wait()

    def step(i, carry):
        @pl.when(i < steps)
        def _():
            by, half = slot(i)
            first = (i >= 1) & (i <= 2)

            @pl.when(first & (z > 0))
            def _():
                arrived(left_slot, half)

            @pl.when(first & (z > 0) & (z < 3))
            def _():
                on_right(half).start()

            @pl.when(first & (z < 3))
            def _():
                arrived(right_slot, half)

            @pl.when(first & (z > 0) & (z < 3))
            def _():
                on_left(half).start()

            second = (i >= 3) & (i <= 4)

            @pl.when(second)
            def _():
                arrived(2, half)

            @pl.when(second & (z > 0) & (z < 3))
            def _():
                to_end(half).start()

            @pl.when((i >= 5) & (i <= 6) & (z != 1) & (z != 2))
            def _():
                arrived(3, half)

            def product(t, carry):
                part = jnp.dot(xall[by, half], w_in[t], preferred_element_type=F32).astype(BF)
                for side in range(2):
                    block = slice(side * piece_rows, (side + 1) * piece_rows)
                    pbuf[side, 0, t] = part[block, :half_cols]
                    pbuf[side, 1, t] = part[block, half_cols:]
                return carry

            lax.fori_loop(0, 3, product, 0)
            core_copy(i).start()
            core_copy(i).wait()

            def add(t, carry):
                for side in range(2):
                    sbuf[i % 2, side, t] = (pbuf[core, side, t].astype(F32) + r1[i % 2, side, t].astype(F32)).astype(BF)
                return carry

            lax.fori_loop(0, 3, add, 0)
            y_copy(i).start()

        @pl.when((i >= 1) & (i <= steps))
        def _():
            j = i - 1
            by, half = slot(j)
            y_copy(j).wait()
            for h in range(heads):
                cols = slice(h * HEAD_DIM, (h + 1) * HEAD_DIM)

                def total(n):
                    return (sbuf[j % 2, ypos, n, :, cols].astype(F32) + r2[j % 3, n, :, cols].astype(F32)).astype(BF)

                def turned(vals):
                    vals = vals.astype(F32)
                    return (vals * cos_ref[half, core] + pltpu.roll(vals, HEAD_DIM // 2, 1) * sin_ref[half, core]).astype(BF)

                qbuf[:, cols] = turned(total(0))
                kvbuf[by, half, core, 0, :, cols] = turned(total(1))
                kvbuf[by, half, core, 1, :, cols] = total(2)
            kv_copy(j).start()
            kv_copy(j).wait()

            def attend(n_halves):
                n_keys = n_halves * rows
                q_pos = (n_halves - 1) * rows + core * piece_rows + lax.broadcasted_iota(jnp.int32, (piece_rows, n_keys), 0)
                allowed = q_pos >= lax.broadcasted_iota(jnp.int32, (piece_rows, n_keys), 1)
                for h in range(heads):
                    cols = slice(h * HEAD_DIM, (h + 1) * HEAD_DIM)
                    keys = kvbuf[by, :n_halves, :, 0, :, cols].reshape(n_keys, HEAD_DIM)
                    vals = kvbuf[by, :n_halves, :, 1, :, cols].reshape(n_keys, HEAD_DIM)
                    scores = lax.dot_general(qbuf[:, cols], keys, (((1,), (1,)), ((), ())), preferred_element_type=F32) * HEAD_DIM ** -0.5
                    scores = jnp.where(allowed, scores, -1e30)
                    weight = jnp.exp(scores - jnp.max(scores, axis=1, keepdims=True))
                    prob = (weight / jnp.sum(weight, axis=1, keepdims=True)).astype(BF)
                    abuf[j % 3, core, ypos, :, cols] = jnp.dot(prob, vals, preferred_element_type=F32).astype(BF)

            @pl.when(half == 0)
            def _():
                attend(1)

            @pl.when(half == 1)
            def _():
                attend(2)

            out_y_copy(j).start()

        @pl.when(i >= 2)
        def _():
            j = i - 2
            by, half = slot(j)
            out_y_copy(j).wait()
            out_core_copy(j).start()

            @pl.when((inner == 0) & (j >= 3) & (j < steps - 1))
            def _():
                direct_copy(j - 2).wait_send()

            out_core_copy(j).wait()

            def out(t, carry):
                cols = pl.ds(pl.multiple_of(t * 256, 256), 256)
                part = jnp.dot(abuf[j % 3, :, 0].reshape(rows, half_cols), w_out[0:half_cols, cols], preferred_element_type=F32)
                part += jnp.dot(abuf[j % 3, :, 1].reshape(rows, half_cols), w_out[half_cols:, cols], preferred_element_type=F32)

                @pl.when(by == 0)
                def _():
                    own[half, :, cols] = part

                @pl.when((by > 0) & ((inner == 0) | (j > 4)))
                def _():
                    zsend[j % 2, :, cols] = part.astype(BF)

                @pl.when((by > 0) & (inner == 1) & (j <= 4))
                def _():
                    cbuf[((j + 1) // 2 + 1) % 2, half, :, cols] = part.astype(BF)
                return carry

            lax.fori_loop(0, width // 256, out, 0)

            @pl.when(((inner == 0) & (j >= 1) & (j <= 2)) | ((inner == 1) & (j >= 5) & (j <= 6)))
            def _():
                direct_copy(j).start()

            @pl.when((inner == 0) & (j >= 3) & (j <= 6))
            def _():
                relay_copy(j).start()

        @pl.when((inner == 1) & (i == steps - 1))
        def _():
            combine(0, 0)

        @pl.when((inner == 1) & (i == steps))
        def _():
            combine(0, 1)
        return carry

    lax.fori_loop(0, steps + 2, step, 0)

    for half in range(halves):
        @pl.when(z < 3)
        def _():
            to_right(half).wait_send()

        @pl.when(z > 0)
        def _():
            to_left(half).wait_send()

        @pl.when((z > 0) & (z < 3))
        def _():
            on_right(half).wait_send()
            on_left(half).wait_send()
            to_end(half).wait_send()

    @pl.when(inner == 1)
    def _():
        combine(1, 0)
        combine(1, 1)

    for j in (steps - 3, steps - 2):
        direct_copy(j).wait_send()
    for half in range(halves):
        @pl.when(inner == 1)
        def _():
            cross_copy(0, half).wait_send()
            cross_copy(1, half).wait_send()

        for source in range(2):
            remote(zsend.at[0], zrecv.at[source, half], zr_send.at[0], zr_recv.at[source, half], {"ty": flip(z, 1)}).wait_recv()

        def finish(t, carry):
            part = pl.ds(pl.multiple_of(t * 32, 32), 32)
            total = own[half, part]
            for source in range(2):
                total += zrecv[source, half, part].astype(F32)
            out_ref[half, part] = (x_ref[half, part].astype(F32) + total.astype(BF).astype(F32)).astype(BF)
            return carry

        lax.fori_loop(0, rows // 32, finish, 0)


def attention(x, w_q, w_k, w_v, w_o):
    seq_len, width = x.shape
    rows, half_cols = seq_len // 2, width // 2
    piece_rows = rows // 2
    cos_t, sin_t = rot_tables(seq_len)
    dma, vmem = pltpu.SemaphoreType.DMA, pltpu.VMEM
    in_vmem, anywhere = pl.BlockSpec(memory_space=pltpu.VMEM), pl.BlockSpec(memory_space=pl.ANY)
    out = pl.pallas_call(
        attn_kernel,
        name="attention",
        out_shape=jax.ShapeDtypeStruct((2, rows, width), BF),
        in_specs=[in_vmem] * 3 + [anywhere] * 4,
        out_specs=in_vmem,
        scratch_shapes=[
            vmem((4, 2, rows, width), BF),
            vmem((3, width, width), BF),
            vmem((width, width), BF),
            vmem((2, 2, 3, piece_rows, half_cols), BF),
            vmem((2, 2, 3, piece_rows, half_cols), BF),
            vmem((2, 2, 3, piece_rows, half_cols), BF),
            vmem((3, 3, piece_rows, half_cols), BF),
            vmem((piece_rows, half_cols), BF),
            vmem((4, 2, 2, 2, piece_rows, half_cols), BF),
            vmem((3, 2, 2, piece_rows, half_cols), BF),
            vmem((2, rows, width), BF),
            vmem((2, 2, rows, width), BF),
            vmem((2, 2, rows, width), BF),
            vmem((2, 2, rows, width), BF),
            vmem((2, rows, width), F32),
            vmem((4, 8, seq_len), F32), dma((2,)), dma((2,)),
            dma((4,)), dma((5, 2)), dma((4, 2)),
            dma((2,)), dma((2,)), dma((3,)), dma((3,)), dma((4, 2)), dma((4, 2)),
            dma((3,)), dma((3,)), dma((3,)), dma((3,)),
            dma((2,)), dma((2, 2)), dma((2, 2)), dma((2, 2)),
        ],
        compiler_params=pltpu.CompilerParams(collective_id=1, has_side_effects=True, vmem_limit_bytes=VMEM_LIMIT),
    )(x.reshape(2, rows, width), jnp.asarray(cos_t).reshape(2, 2, piece_rows, HEAD_DIM), jnp.asarray(sin_t).reshape(2, 2, piece_rows, HEAD_DIM), w_q, w_k, w_v, w_o)
    return out.reshape(seq_len, width)


def mlp_kernel(h_ref, wg_hbm, wu_hbm, wd_hbm, out_ref, xall, w_in, w_out, pbuf, r1, sbuf, r2, abuf, zsend, zrecv, own,
               stats, s_send, s_recv, w_sem, az_send, az_recv, p_send, p_recv, ry_send, ry_recv, ay_send, ay_recv, ac_send, ac_recv, zr_send, zr_recv):
    z, me = lax.axis_index("ty"), lax.axis_index("tx")
    core, ypos = me % 2, me // 2
    core_peer, y_peer = {"tx": flip(me, 1)}, {"tx": flip(me, 2)}
    halves, rows, width = h_ref.shape
    ff = wg_hbm.shape[1]
    tiles = ff // TILE
    all_tiles = 2 * tiles
    quarter = rows // 4
    steps = 4 * halves
    pairs = ((0, (tiles + 1) // 2), ((tiles + 1) // 2, tiles))

    def slot(i):
        return ((i + 1) // 2) % 4, (i + 1) % 2

    right_slot, left_slot = 1 + 2 * (z % 2), 3 - 2 * (z % 2)

    def to_right(half):
        return remote(xall.at[0, half], xall.at[right_slot, half], az_send.at[0, half], az_recv.at[right_slot, half], {"ty": (z + 1) % 4})

    def to_left(half):
        return remote(xall.at[0, half], xall.at[left_slot, half], az_send.at[1, half], az_recv.at[left_slot, half], {"ty": (z + 3) % 4})

    def on_right(half):
        return remote(xall.at[left_slot, half], xall.at[2, half], az_send.at[2, half], az_recv.at[2, half], {"ty": (z + 1) % 4})

    def on_left(half):
        return remote(xall.at[right_slot, half], xall.at[2, half], az_send.at[3, half], az_recv.at[2, half], {"ty": (z + 3) % 4})

    def to_end(half):
        return remote(xall.at[2, half], xall.at[3, half], az_send.at[4, half], az_recv.at[3, half], {"ty": (3 * z + 1) % 4})

    def arrived(by, half):
        remote(xall.at[by, half], xall.at[by, half], az_send.at[0, half], az_recv.at[by, half], {"ty": flip(z, 1)}).wait_recv()

    def core_copy(i, part):
        group = pl.ds(2 * pairs[part][0], 2 * (pairs[part][1] - pairs[part][0]))
        return remote(pbuf.at[1 - core, group], r1.at[i % 2, group], p_send.at[i % 2, part], p_recv.at[i % 2, part], core_peer)

    def y_copy(i, part):
        group = pl.ds(2 * pairs[part][0], 2 * (pairs[part][1] - pairs[part][0]))
        return remote(sbuf.at[i % 2, 1 - ypos, group], r2.at[i % 3, group], ry_send.at[i % 3, part], ry_recv.at[i % 3, part], y_peer)

    def act_y_copy(i, part):
        cols = pl.ds(pairs[part][0] * TILE, (pairs[part][1] - pairs[part][0]) * TILE)
        piece = abuf.at[i % 3, core, ypos, :, cols]
        return remote(piece, piece, ay_send.at[i % 3, part], ay_recv.at[i % 3, part], y_peer)

    def act_core_copy(i):
        piece = abuf.at[i % 3, core]
        return remote(piece, piece, ac_send.at[i % 3], ac_recv.at[i % 3], core_peer)

    def scatter_copy(i):
        by, half = slot(i)
        return remote(zsend.at[i % 2], zrecv.at[by - 1, half], zr_send.at[i % 2], zr_recv.at[by - 1, half], {"ty": flip(z, by)})

    loads = [
        pltpu.make_async_copy(wg_hbm, w_in.at[:, pl.ds(0, ff)], w_sem.at[0]),
        pltpu.make_async_copy(wu_hbm, w_in.at[:, pl.ds(ff, ff)], w_sem.at[1]),
        pltpu.make_async_copy(wd_hbm, w_out, w_sem.at[2]),
    ]
    for load in loads:
        load.start()
    greet(z, me)

    def send_own(half):
        @pl.when(z < 3)
        def _():
            to_right(half).start()

        @pl.when(z > 0)
        def _():
            to_left(half).start()

    norm_rows(h_ref, xall.at[0], stats, s_send, s_recv, core_peer, y_peer, send_own)
    loads[0].wait()
    loads[1].wait()

    def step(i, carry):
        @pl.when(i < steps)
        def _():
            by, half = slot(i)

            first = (i >= 1) & (i <= 2)

            @pl.when(first & (z > 0))
            def _():
                arrived(left_slot, half)

            @pl.when(first & (z > 0) & (z < 3))
            def _():
                on_right(half).start()

            @pl.when(first & (z < 3))
            def _():
                arrived(right_slot, half)

            @pl.when(first & (z > 0) & (z < 3))
            def _():
                on_left(half).start()

            second = (i >= 3) & (i <= 4)

            @pl.when(second)
            def _():
                arrived(2, half)

            @pl.when(second & (z > 0) & (z < 3))
            def _():
                to_end(half).start()

            @pl.when((i >= 5) & (i <= 6) & (z != 1) & (z != 2))
            def _():
                arrived(3, half)

            def product(t, carry):
                for side in range(2):
                    cols = pl.ds(pl.multiple_of(side * ff + t * TILE, TILE), TILE)
                    part = jnp.dot(xall[by, half], w_in[:, cols], preferred_element_type=F32).astype(BF)
                    pbuf[:, 2 * t + side] = part.reshape(2, 2, quarter, TILE)
                return carry

            for part in range(2):
                lax.fori_loop(*pairs[part], product, 0)
                core_copy(i, part).start()
            for part in range(2):
                core_copy(i, part).wait_recv()

                def add(t, carry):
                    total = pbuf[core, t].astype(F32) + r1[i % 2, t].astype(F32)
                    total = total.astype(BF)
                    sbuf[i % 2, 0, t] = total[0]
                    sbuf[i % 2, 1, t] = total[1]
                    return carry

                lax.fori_loop(2 * pairs[part][0], 2 * pairs[part][1], add, 0)
                y_copy(i, part).start()
            for part in range(2):
                core_copy(i, part).wait_send()

        @pl.when((i >= 1) & (i <= steps))
        def _():
            j = i - 1

            def gate(t, carry):
                g = (sbuf[j % 2, ypos, 2 * t].astype(F32) + r2[j % 3, 2 * t].astype(F32)).astype(BF).astype(F32)
                u = (sbuf[j % 2, ypos, 2 * t + 1].astype(F32) + r2[j % 3, 2 * t + 1].astype(F32)).astype(BF).astype(F32)
                cols = pl.ds(pl.multiple_of(t * TILE, TILE), TILE)
                abuf[j % 3, core, ypos, :, cols] = (g * jax.nn.sigmoid(g) * u).astype(BF)
                return carry

            for part in range(2):
                y_copy(j, part).wait()
                lax.fori_loop(*pairs[part], gate, 0)
                act_y_copy(j, part).start()

        @pl.when(i >= 2)
        def _():
            j = i - 2
            by, half = slot(j)
            act_y_copy(j, 0).wait()
            act_y_copy(j, 1).wait()
            act_core_copy(j).start()

            @pl.when(j == 0)
            def _():
                loads[2].wait()

            @pl.when((j >= 3) & (j < steps - 1))
            def _():
                scatter_copy(j - 2).wait_send()

            act_core_copy(j).wait()

            def down(t, carry):
                cols = pl.ds(pl.multiple_of(t * 256, 256), 256)
                part = jnp.dot(abuf[j % 3].reshape(rows, ff), w_out[:, cols], preferred_element_type=F32)

                @pl.when(by == 0)
                def _():
                    own[half, :, cols] = part

                @pl.when(by > 0)
                def _():
                    zsend[j % 2, :, cols] = part.astype(BF)
                return carry

            lax.fori_loop(0, width // 256, down, 0)

            @pl.when(by > 0)
            def _():
                scatter_copy(j).start()
        return carry

    lax.fori_loop(0, steps + 2, step, 0)

    for half in range(halves):
        @pl.when(z < 3)
        def _():
            to_right(half).wait_send()

        @pl.when(z > 0)
        def _():
            to_left(half).wait_send()

        @pl.when((z > 0) & (z < 3))
        def _():
            on_right(half).wait_send()
            on_left(half).wait_send()
            to_end(half).wait_send()

    for j in (steps - 3, steps - 2):
        scatter_copy(j).wait_send()
    for half in range(halves):
        for by in (1, 2, 3):
            remote(zsend.at[0], zrecv.at[by - 1, half], zr_send.at[0], zr_recv.at[by - 1, half], {"ty": flip(z, by)}).wait_recv()

        def finish(t, carry):
            part = pl.ds(pl.multiple_of(t * 32, 32), 32)
            total = own[half, part]
            for by in range(3):
                total += zrecv[by, half, part].astype(F32)
            out_ref[half, part] = (h_ref[half, part].astype(F32) + total.astype(BF).astype(F32)).astype(BF)
            return carry

        lax.fori_loop(0, rows // 32, finish, 0)


def mlp(h, w_gate, w_up, w_down):
    seq_len, width = h.shape
    ff = w_gate.shape[1]
    halves = 2
    rows = seq_len // halves
    quarter = rows // 4
    tiles = ff // TILE
    dma, vmem = pltpu.SemaphoreType.DMA, pltpu.VMEM
    in_vmem, anywhere = pl.BlockSpec(memory_space=pltpu.VMEM), pl.BlockSpec(memory_space=pl.ANY)
    out = pl.pallas_call(
        mlp_kernel,
        name="mlp",
        out_shape=jax.ShapeDtypeStruct((halves, rows, width), BF),
        in_specs=[in_vmem, anywhere, anywhere, anywhere],
        out_specs=in_vmem,
        scratch_shapes=[
            vmem((4, halves, rows, width), BF),
            vmem((width, 2 * ff), BF),
            vmem((ff, width), BF),
            vmem((2, 2 * tiles, 2, quarter, TILE), BF),
            vmem((2, 2 * tiles, 2, quarter, TILE), BF),
            vmem((2, 2, 2 * tiles, quarter, TILE), BF),
            vmem((3, 2 * tiles, quarter, TILE), BF),
            vmem((3, 2, 2, quarter, ff), BF),
            vmem((2, rows, width), BF),
            vmem((3, halves, rows, width), BF),
            vmem((halves, rows, width), F32),
            vmem((4, 8, seq_len), F32), dma((2,)), dma((2,)),
            dma((3,)), dma((5, halves)), dma((4, halves)),
            dma((2, 2)), dma((2, 2)), dma((3, 2)), dma((3, 2)),
            dma((3, 2)), dma((3, 2)), dma((3,)), dma((3,)),
            dma((2,)), dma((3, halves)),
        ],
        compiler_params=pltpu.CompilerParams(collective_id=0, has_side_effects=True, vmem_limit_bytes=VMEM_LIMIT),
    )(h.reshape(halves, rows, width), w_gate, w_up, w_down)
    return out.reshape(seq_len, width)


def solution(mesh):
    act_spec = P(("dp", "ty"), None, "tx")
    col_spec = P("tx", "ty")
    row_spec = P("ty", "tx")

    def layer_fn(x_blk, w_q, w_k, w_v, w_o, w_gate, w_up, w_down):
        h = attention(x_blk[0], w_q, w_k, w_v, w_o)
        return mlp(h, w_gate, w_up, w_down)[None]

    return jax.shard_map(layer_fn, mesh=mesh, in_specs=(act_spec, col_spec, col_spec, col_spec, row_spec, col_spec, col_spec, row_spec), out_specs=act_spec, check_vma=False)
```
